128 devices in a mesh: seq: 16 (over x_hi, z, core), res: 8 (over x_lo, y).
Axes of the slice: x: 4 (x_hi: 2, x_lo: 2; x = x_hi * 2 + x_lo), y: 4, z: 4, core: 2. Of those that a mesh axis runs over, the one named last changes fastest.
Arguments:
- alignment_embedding: bfloat16 [128, 2048, 256], P('seq', 'res'), may hold values from -6 to 6
- unscaled_edge_prior: bfloat16 [8, 2048, 2048], P(None, 'res', 'seq'), may hold values from -6 to 6
- edge_prior_factor: float32 [8], replicated, may hold values from 0.5 to 3
- horizontal_standardize_factor: float32 [256], replicated, may hold values from 0.25 to 1.75
- horizontal_probe_lookup: bfloat16 [2, 256, 256], replicated, may hold values from -15 to 15
- horizontal_content_switch: bfloat16 [2, 256, 256], replicated, may hold values from -0.375 to 0.375
- horizontal_sigmoid_shift: float32 [256], replicated, may hold values from -4 to 4
- horizontal_final_matrix: bfloat16 [256, 256], replicated, may hold values from -0.375 to 0.375
- vertical_standardize_factor: float32 [256], replicated, may hold values from 0.25 to 1.75
- vertical_probe_lookup: bfloat16 [2, 256, 256], replicated, may hold values from -15 to 15
- vertical_content_switch: bfloat16 [2, 256, 256], replicated, may hold values from -0.375 to 0.375
- vertical_sigmoid_shift: float32 [256], replicated, may hold values from -4 to 4
- vertical_final_matrix: bfloat16 [256, 256], replicated, may hold values from -0.375 to 0.375
Outputs:
- msa_out: float32 [128, 2048, 256], P('seq', 'res')
The draws below stay inside these ranges and needn't reach their ends.
All inputs are finite; a program needn't handle non-finite values.
Results may differ from the reference program's by a relative error of at most 0.04.
The reference program's roundings to bfloat16 on the way count: a program that leaves them out, or rounds other values in their place, can miss the bound.
Values may be sent and summed in bfloat16 or wider, within the bound.
A program may use at most 128 MiB of HBM per device.

```python
import math
import jax
import jax.numpy as jnp
from jax import lax

FEATURE_DEPTH = 256
LEARNER_NUMBER = 8
SUBSPACE_WIDTH = 32
ALIGNED_AMOUNT = 128
POSITION_AMOUNT = 2048


def qk_pair(key, deviation):
    starting_point = jax.random.normal(key, (2, FEATURE_DEPTH, LEARNER_NUMBER * SUBSPACE_WIDTH), jnp.float32) * (deviation / math.sqrt(FEATURE_DEPTH))
    starting_point = jnp.clip(starting_point, -6.0 * deviation / math.sqrt(FEATURE_DEPTH), 6.0 * deviation / math.sqrt(FEATURE_DEPTH))
    return starting_point.astype(jnp.bfloat16)


def draw_horizontal_probe_lookup(key, part):
    return qk_pair(jax.random.fold_in(key, 11), 1.5)


def draw_vertical_probe_lookup(key, part):
    return qk_pair(jax.random.fold_in(key, 13), 2.5)


def levels(stream_key, dims, pieces, low, top_value):
    gain, own = 1.0, jax.random.fold_in(stream_key, 6)
    for dim, blocks in pieces:
        steps = jnp.exp(jax.random.uniform(jax.random.fold_in(own, dim), (blocks,), jnp.float32, low / len(pieces), top_value / len(pieces)))
        gain = gain * jnp.repeat(steps, dims[dim] // blocks).reshape([-1 if axis == dim else 1 for axis in range(len(dims))])
    return gain


def gaussian(key, dims, scale, limit, split=(), kind=jnp.bfloat16):
    gain = levels(key, dims, split, -0.22, 0.18) if split else 1.0
    drawn = jax.random.normal(key, dims, jnp.float32) * scale * gain
    return jnp.minimum(jnp.maximum(drawn, -limit), limit).astype(kind)


def setup_inputs(seed: int = 0) -> dict:
    arg_keys = jax.random.split(jax.random.key(seed), 14)
    alignment_embedding = gaussian(arg_keys[0], (ALIGNED_AMOUNT, POSITION_AMOUNT, FEATURE_DEPTH), 1.0, 6.0, ((0, 16), (1, 8)))
    unscaled_edge_prior = gaussian(arg_keys[1], (LEARNER_NUMBER, POSITION_AMOUNT, POSITION_AMOUNT), 1.0, 6.0, ((1, 8), (2, 16)))
    edge_prior_factor = jnp.clip(jnp.exp(jax.random.uniform(arg_keys[2], (LEARNER_NUMBER,), jnp.float32, math.log(0.5), math.log(3.0))), 0.5, 3.0)
    horizontal_standardize_factor = jnp.clip(1.0 + 0.15 * jax.random.normal(arg_keys[3], (FEATURE_DEPTH,), jnp.float32), 0.25, 1.75)
    horizontal_probe_lookup = draw_horizontal_probe_lookup(jax.random.fold_in(arg_keys[13], 71), 0)
    horizontal_content_switch = gaussian(arg_keys[5], (2, FEATURE_DEPTH, LEARNER_NUMBER * SUBSPACE_WIDTH), FEATURE_DEPTH ** -0.5, 0.375)
    horizontal_sigmoid_shift = gaussian(arg_keys[6], (LEARNER_NUMBER * SUBSPACE_WIDTH,), 1.0, 4.0, (), jnp.float32)
    horizontal_final_matrix = gaussian(arg_keys[7], (LEARNER_NUMBER * SUBSPACE_WIDTH, FEATURE_DEPTH), (LEARNER_NUMBER * SUBSPACE_WIDTH) ** -0.5, 0.375)
    vertical_standardize_factor = jnp.clip(1.0 + 0.15 * jax.random.normal(arg_keys[8], (FEATURE_DEPTH,), jnp.float32), 0.25, 1.75)
    vertical_probe_lookup = draw_vertical_probe_lookup(jax.random.fold_in(arg_keys[13], 71), 0)
    vertical_content_switch = gaussian(arg_keys[10], (2, FEATURE_DEPTH, LEARNER_NUMBER * SUBSPACE_WIDTH), FEATURE_DEPTH ** -0.5, 0.375)
    vertical_sigmoid_shift = gaussian(arg_keys[11], (LEARNER_NUMBER * SUBSPACE_WIDTH,), 1.0, 4.0, (), jnp.float32)
    vertical_final_matrix = gaussian(arg_keys[12], (LEARNER_NUMBER * SUBSPACE_WIDTH, FEATURE_DEPTH), (LEARNER_NUMBER * SUBSPACE_WIDTH) ** -0.5, 0.375)
    return dict(alignment_embedding=alignment_embedding, unscaled_edge_prior=unscaled_edge_prior, edge_prior_factor=edge_prior_factor, horizontal_standardize_factor=horizontal_standardize_factor, horizontal_probe_lookup=horizontal_probe_lookup, horizontal_content_switch=horizontal_content_switch, horizontal_sigmoid_shift=horizontal_sigmoid_shift, horizontal_final_matrix=horizontal_final_matrix, vertical_standardize_factor=vertical_standardize_factor, vertical_probe_lookup=vertical_probe_lookup, vertical_content_switch=vertical_content_switch, vertical_sigmoid_shift=vertical_sigmoid_shift, vertical_final_matrix=vertical_final_matrix)


EPS = 1e-05

def lower_precision(array):
    return lax.optimization_barrier(array.astype(jnp.bfloat16))

def standardize_features(row_data, standardize_factor):
    row_data = row_data.astype(jnp.float32)
    row_mean = lax.optimization_barrier(jnp.mean(row_data, -1, keepdims=True))
    centred = row_data - row_mean
    deviation = lax.optimization_barrier(jnp.mean(centred * centred, -1, keepdims=True))
    return lower_precision(centred * lax.rsqrt(deviation + EPS) * standardize_factor)

def linear_transform(array, weight):
    return jnp.einsum('...c,cf->...f', array.astype(jnp.float32), weight.astype(jnp.float32))

def horizontal_focus_path(alignment_embedding, unscaled_edge_prior, edge_prior_factor, standardize_factor, probe_lookup_matrix, content_switch_matrix, sigmoid_shift_array, final_matrix):
    position_number = alignment_embedding.shape[1]
    head_count = edge_prior_factor.shape[0]
    proj_width = probe_lookup_matrix.shape[2]
    head_size = proj_width // head_count
    scaled_bias = unscaled_edge_prior.astype(jnp.float32) * edge_prior_factor[:, None, None]
    standardized_source = standardize_features(alignment_embedding, standardize_factor)

    def one_sequence(seq_rows):
        queries = lower_precision(linear_transform(seq_rows, probe_lookup_matrix[0])).reshape(position_number, head_count, head_size)
        key_part = lower_precision(linear_transform(seq_rows, probe_lookup_matrix[1])).reshape(position_number, head_count, head_size)
        values = lower_precision(linear_transform(seq_rows, content_switch_matrix[0])).reshape(position_number, head_count, head_size)
        gates = jax.nn.sigmoid(linear_transform(seq_rows, content_switch_matrix[1]) + sigmoid_shift_array)
        scores = jnp.einsum('ihd,jhd->hij', queries.astype(jnp.float32), key_part.astype(jnp.float32)) / math.sqrt(head_size) + scaled_bias
        row_max = lax.optimization_barrier(jnp.max(scores, -1, keepdims=True))
        weights = jnp.exp(scores - row_max)
        totals = lax.optimization_barrier(jnp.sum(weights, -1))
        focused_result = jnp.einsum('hij,jhd->ihd', lower_precision(weights).astype(jnp.float32), values.astype(jnp.float32)) / totals.T[:, :, None]
        return lower_precision(focused_result.reshape(position_number, proj_width) * gates)
    focused_result = lax.map(one_sequence, standardized_source)
    return alignment_embedding.astype(jnp.float32) + linear_transform(focused_result, final_matrix)

def column_branch(combined_subspaces, standardize_factor, probe_lookup_matrix, content_switch_matrix, sigmoid_shift_array, final_matrix, head_count):
    seq_total, position_number, feature_number = combined_subspaces.shape
    proj_width = probe_lookup_matrix.shape[2]
    head_size = proj_width // head_count
    blocks = combined_subspaces.transpose(1, 0, 2).reshape(position_number // 16, 16, seq_total, feature_number)

    def one_block(block_rows):
        standardized_source = standardize_features(block_rows, standardize_factor)
        queries = lower_precision(linear_transform(standardized_source, probe_lookup_matrix[0])).reshape(16, seq_total, head_count, head_size)
        key_part = lower_precision(linear_transform(standardized_source, probe_lookup_matrix[1])).reshape(16, seq_total, head_count, head_size)
        values = lower_precision(linear_transform(standardized_source, content_switch_matrix[0])).reshape(16, seq_total, head_count, head_size)
        gates = jax.nn.sigmoid(linear_transform(standardized_source, content_switch_matrix[1]) + sigmoid_shift_array)
        scores = jnp.einsum('rshd,rthd->rhst', queries.astype(jnp.float32), key_part.astype(jnp.float32)) / math.sqrt(head_size)
        row_max = lax.optimization_barrier(jnp.max(scores, -1, keepdims=True))
        weights = jnp.exp(scores - row_max)
        totals = lax.optimization_barrier(jnp.sum(weights, -1))
        focused_result = jnp.einsum('rhst,rthd->rshd', lower_precision(weights).astype(jnp.float32), values.astype(jnp.float32)) / totals.transpose(0, 2, 1)[:, :, :, None]
        focused_result = lower_precision(focused_result.reshape(16, seq_total, proj_width) * gates)
        return block_rows.astype(jnp.float32) + linear_transform(focused_result, final_matrix)
    result = lax.map(one_block, blocks)
    return result.reshape(position_number, seq_total, feature_number).transpose(1, 0, 2)

def reference(alignment_embedding, unscaled_edge_prior, edge_prior_factor, horizontal_standardize_factor, horizontal_probe_lookup, horizontal_content_switch, horizontal_sigmoid_shift, horizontal_final_matrix, vertical_standardize_factor, vertical_probe_lookup, vertical_content_switch, vertical_sigmoid_shift, vertical_final_matrix):
    combined_subspaces = horizontal_focus_path(alignment_embedding, unscaled_edge_prior, edge_prior_factor, horizontal_standardize_factor, horizontal_probe_lookup, horizontal_content_switch, horizontal_sigmoid_shift, horizontal_final_matrix)
    return column_branch(combined_subspaces, vertical_standardize_factor, vertical_probe_lookup, vertical_content_switch, vertical_sigmoid_shift, vertical_final_matrix, edge_prior_factor.shape[0])
```

```python
import functools
import math

import jax
import jax.numpy as jnp
from jax import lax
from jax.experimental import pallas as pl
from jax.experimental.pallas import tpu as pltpu
from jax.sharding import PartitionSpec as P

EPS = 1e-05
LOG2E = 1.4426950408889634
F32 = jnp.float32
BF16 = jnp.bfloat16
HEADS = 8
WIDTH = 32
HALF = 128
VROWS = 48
CHUNK = 256
VM = pltpu.VMEM


def dot_nn(a, b):
    return lax.dot_general(a, b, (((1,), (0,)), ((), ())), preferred_element_type=F32)


def dot_nt(a, b):
    return lax.dot_general(a, b, (((1,), (1,)), ((), ())), preferred_element_type=F32)


def standardize(x, factor):
    mean = jnp.sum(x, -1, keepdims=True) * (1.0 / x.shape[-1])
    centred = x - mean
    var = jnp.sum(centred * centred, -1, keepdims=True) * (1.0 / x.shape[-1])
    return centred * lax.rsqrt(var + EPS) * factor


def row_kernel(
    x_ref, rows_ref, panel_ref, factor_ref, probe_ref, switch_ref, shift_ref, final_ref,
    mixed_ref,
    bias_ref, even_ref, odd_ref, key_ref, value_ref, query_ref, probe_t_ref, switch_t_ref, att_ref,
    max_ref,
):
    sequences, positions, depth = x_ref.shape
    keys = rows_ref.shape[1]
    chunks = keys // CHUNK
    res = lax.axis_index("res")
    probe_t_ref[...] = probe_ref[0].astype(F32).T.astype(BF16)
    switch_t_ref[...] = switch_ref[0].astype(F32).T.astype(BF16)
    query_ref[...] = jnp.zeros_like(query_ref)
    scale = LOG2E / math.sqrt(WIDTH)

    @pl.loop(0, HEADS)
    def _(head):
        value_ref[head, WIDTH:, :] = jnp.ones((VROWS - WIDTH, keys), BF16)

        @pl.loop(0, chunks)
        def _(c):
            at = pl.ds(pl.multiple_of(c * CHUNK, CHUNK), CHUNK)
            bias_ref[head, at, :] = panel_ref[head, at, :].astype(F32) * (factor_ref[head] * LOG2E)

    def scores(head, into, c):
        at = pl.ds(c * CHUNK, CHUNK)
        part = dot_nn(key_ref[head // 4, at, :], query_ref[head]) + bias_ref[head, at, :]
        into[at, :] = part
        return jnp.max(part.reshape(CHUNK // 8, 8, positions), axis=0)

    def step(head, following, source, into, top):
        total = jnp.zeros((VROWS, positions), F32)
        top_next = None
        for c in range(chunks):
            at = pl.ds(c * CHUNK, CHUNK)
            high = scores(following, into, c)
            top_next = high if top_next is None else jnp.maximum(top_next, high)
            weight = jnp.exp2(source[at, :] - top).astype(BF16)
            total = total + dot_nn(value_ref[head, :, at], weight)
        att_ref[pl.ds(pl.multiple_of(head * WIDTH, WIDTH), WIDTH), :] = (
            total[:WIDTH] / total[WIDTH : WIDTH + 1]
        )
        return jnp.max(top_next, axis=0, keepdims=True)

    @pl.loop(0, sequences)
    def _(s):
        own = rows_ref[s, pl.ds(pl.multiple_of(res * positions, positions), positions), :]

        @pl.loop(0, chunks // 4)
        def _(group):
            for k in range(4):
                at = pl.ds(pl.multiple_of(group * (4 * CHUNK) + k * CHUNK, CHUNK), CHUNK)
                part = rows_ref[s, at, :]
                key = dot_nn(part, probe_ref[1]).astype(BF16)
                key_ref[0, at, :] = key[:, :HALF]
                key_ref[1, at, :] = key[:, HALF:]
                value = dot_nt(switch_t_ref[...], part).astype(BF16)
                for head in range(HEADS):
                    value_ref[head, :WIDTH, at] = value[head * WIDTH : (head + 1) * WIDTH]

        query = (dot_nt(probe_t_ref[...], own) * scale).astype(BF16)
        for head in range(HEADS):
            low = head % 4 * WIDTH
            query_ref[head, low : low + WIDTH, :] = query[head * WIDTH : (head + 1) * WIDTH]
        top = scores(0, even_ref, 0)
        for c in range(1, chunks):
            top = jnp.maximum(top, scores(0, even_ref, c))
        max_ref[...] = jnp.max(top, axis=0, keepdims=True)

        @pl.loop(0, HEADS // 2)
        def _(pair):
            head = pair * 2
            top = step(head, head + 1, even_ref, odd_ref, max_ref[...])
            max_ref[...] = step(head + 1, lax.rem(head + 2, HEADS), odd_ref, even_ref, top)

        gates = jax.nn.sigmoid(dot_nn(own, switch_ref[1]) + shift_ref[...])
        attended = (att_ref[...].T * gates).astype(BF16)
        mixed_ref[s] = x_ref[s].astype(F32) + dot_nn(attended, final_ref[...])


def row_attention(x, rows, panel, factor, probe, switch, shift, final):
    sequences, positions, depth = x.shape
    keys = rows.shape[1]
    vmem = pl.BlockSpec(memory_space=VM)
    return pl.pallas_call(
        row_kernel,
        out_shape=jax.ShapeDtypeStruct(x.shape, F32),
        in_specs=[vmem, vmem, vmem, pl.BlockSpec(memory_space=pltpu.SMEM)] + [vmem] * 4,
        out_specs=vmem,
        scratch_shapes=[
            VM((HEADS, keys, positions), F32),
            VM((keys, positions), F32),
            VM((keys, positions), F32),
            VM((2, keys, HALF), BF16),
            VM((HEADS, VROWS, keys), BF16),
            VM((HEADS, HALF, positions), BF16),
            VM((depth, depth), BF16),
            VM((depth, depth), BF16),
            VM((depth, positions), F32),
            VM((1, positions), F32),
        ],
        compiler_params=pltpu.CompilerParams(vmem_limit_bytes=66_000_000),
    )(x, rows, panel, factor, probe, switch, shift[None], final)


def column_kernel(
    rows_ref, norm_ref, probe_ref, switch_ref, shift_ref, final_ref,
    out_ref,
    left_ref, right_ref, probe_t_ref, switch_t_ref, query_ref, att_ref,
):
    count, residues, depth = rows_ref.shape
    probe_t_ref[...] = probe_ref[0].astype(F32).T.astype(BF16)
    switch_t_ref[...] = switch_ref[0].astype(F32).T.astype(BF16)
    query_ref[...] = jnp.zeros_like(query_ref)
    scale = LOG2E / math.sqrt(WIDTH)
    step = 16

    @pl.loop(0, count // step)
    def _(i):
        part = rows_ref[pl.ds(pl.multiple_of(i * step, step), step)].astype(F32)
        part = part.reshape(step * residues, depth)
        rows = step * residues
        part = standardize(part, norm_ref[...])
        at = pl.ds(pl.multiple_of(i * rows, rows), rows)
        left_ref[at, :] = part[:, :HALF]
        right_ref[at, :] = part[:, HALF:]

    @pl.loop(0, residues)
    def _(r):
        spots = pl.ds(r, count, stride=residues)
        normed = jnp.concatenate([left_ref[spots, :], right_ref[spots, :]], axis=1).astype(BF16)
        key = dot_nn(normed, probe_ref[1]).astype(BF16)
        query = (dot_nt(probe_t_ref[...], normed) * scale).astype(BF16)
        value = dot_nt(switch_t_ref[...], normed).astype(BF16)
        gates = jax.nn.sigmoid(dot_nn(normed, switch_ref[1]) + shift_ref[...])
        ones = jnp.ones((16, count), BF16)
        for half in range(2):
            for k in range(4):
                low = k * WIDTH
                query_ref[low : low + WIDTH, k * count : (k + 1) * count] = query[
                    half * HALF + low : half * HALF + low + WIDTH
                ]
            score = dot_nn(key[:, half * HALF : (half + 1) * HALF], query_ref[...])
            top = jnp.max(score, axis=0, keepdims=True)
            weight = jnp.exp2(score - top).astype(BF16)
            for k in range(4):
                low = half * HALF + k * WIDTH
                block = jnp.concatenate([value[low : low + WIDTH], ones], axis=0)
                total = dot_nn(block, weight[:, k * count : (k + 1) * count])
                att_ref[low : low + WIDTH, :] = total[:WIDTH] / total[WIDTH : WIDTH + 1]
        attended = (att_ref[...].T * gates).astype(BF16)
        delta = dot_nn(attended, final_ref[...])
        left_ref[spots, :] = delta[:, :HALF]
        right_ref[spots, :] = delta[:, HALF:]

    @pl.loop(0, count // step)
    def _(i):
        rows = step * residues
        at = pl.ds(pl.multiple_of(i * rows, rows), rows)
        part = jnp.concatenate([left_ref[at, :], right_ref[at, :]], axis=1)
        out_ref[pl.ds(pl.multiple_of(i * step, step), step)] = part.astype(BF16).reshape(
            step, residues, depth
        )


def column_attention(rows, norm, probe, switch, shift, final):
    count, residues, depth = rows.shape
    vmem = pl.BlockSpec(memory_space=VM)
    return pl.pallas_call(
        column_kernel,
        out_shape=jax.ShapeDtypeStruct(rows.shape, BF16),
        in_specs=[vmem] * 6,
        out_specs=vmem,
        scratch_shapes=[
            VM((count * residues, HALF), F32),
            VM((count * residues, HALF), F32),
            VM((depth, depth), BF16),
            VM((depth, depth), BF16),
            VM((HALF, 4 * count), BF16),
            VM((depth, count), F32),
        ],
    )(rows, norm[None], probe, switch, shift[None], final)


def standardize_features(row_data, standardize_factor):
    row_data = row_data.astype(F32)
    row_mean = jnp.mean(row_data, -1, keepdims=True)
    centred = row_data - row_mean
    deviation = jnp.mean(centred * centred, -1, keepdims=True)
    return (centred * lax.rsqrt(deviation + EPS) * standardize_factor).astype(BF16)


def shards(x, prior, factor, norm_h, probe_h, switch_h, shift_h, final_h, norm_v, probe_v, switch_v, shift_v, final_v):
    sequences, positions, depth = x.shape
    normed = standardize_features(x, norm_h)
    panel = lax.all_gather(prior.transpose(0, 2, 1), "seq", axis=1, tiled=True)
    rows = lax.all_gather(normed, "res", axis=1, tiled=True)
    mixed = row_attention(x, rows, panel, factor, probe_h, switch_h, shift_h, final_h)
    seq_count = lax.axis_size("seq")
    slices = positions // seq_count
    layered = mixed.astype(BF16).reshape(sequences, seq_count, slices, depth)
    columns = lax.all_to_all(layered, "seq", split_axis=1, concat_axis=0, tiled=True)
    delta = column_attention(columns[:, 0], norm_v, probe_v, switch_v, shift_v, final_v)
    back = lax.all_to_all(delta[:, None], "seq", split_axis=0, concat_axis=1, tiled=True)
    return mixed + back.reshape(sequences, positions, depth).astype(F32)


def solution(mesh):
    placed = (P("seq", "res", None), P(None, "res", "seq")) + (P(),) * 11
    return jax.shard_map(
        shards, mesh=mesh, in_specs=placed, out_specs=P("seq", "res", None), check_vma=False
    )
```

```python
import functools
import math

import jax
import jax.numpy as jnp
from jax import lax
from jax.experimental import pallas as pl
from jax.experimental.pallas import tpu as pltpu
from jax.sharding import PartitionSpec as P

EPS = 1e-05
LOG2E = 1.4426950408889634
F32 = jnp.float32
BF16 = jnp.bfloat16
HEADS = 8
WIDTH = 32
HALF = 128
VROWS = 48
CHUNK = 256
VM = pltpu.VMEM


def dot_nn(a, b):
    return lax.dot_general(a, b, (((1,), (0,)), ((), ())), preferred_element_type=F32)


def dot_nt(a, b):
    return lax.dot_general(a, b, (((1,), (1,)), ((), ())), preferred_element_type=F32)


def standardize(x, factor):
    mean = jnp.sum(x, -1, keepdims=True) * (1.0 / x.shape[-1])
    centred = x - mean
    var = jnp.sum(centred * centred, -1, keepdims=True) * (1.0 / x.shape[-1])
    return centred * lax.rsqrt(var + EPS) * factor


MESH = pl.DeviceIdType.MESH
RING = 4


class Exchange:
    def __init__(self, axis, cores, view, send, recv):
        index = lax.axis_index(axis)
        self.axis, self.cores, self.view, self.send, self.recv = axis, cores, view, send, recv
        self.core = lax.rem(index, cores)
        chip = index // cores
        self.ring, self.at = chip // RING, lax.rem(chip, RING)
        self.mirror = self.device(1 - self.ring, 0)
        self.up, self.down = self.device(self.ring, 1), self.device(self.ring, -1)

    def block(self, ring, shift):
        return ring * RING + lax.rem(self.at + (shift + RING), RING)

    def device(self, ring, shift):
        return self.block(ring, shift) * self.cores + self.core

    def peers(self):
        return [{self.axis: d} for d in (self.mirror, self.up, self.down)]

    def plan(self, kind):
        mine, other = self.ring, 1 - self.ring
        return {
            0: ((mine, 0, None), self.mirror, (other, 0, None)),
            1: ((mine, 0, None), self.up, (mine, -1, None)),
            2: ((mine, 0, None), self.down, (mine, 1, None)),
            3: ((other, 0, None), self.up, (other, -1, None)),
            4: ((other, 0, None), self.down, (other, 1, None)),
            5: ((mine, -1, 0), self.up, (mine, -2, 0)),
            6: ((mine, 1, 1), self.down, (mine, 2, 1)),
            7: ((other, -1, 0), self.up, (other, -2, 0)),
            8: ((other, 1, 1), self.down, (other, 2, 1)),
            9: ((mine, 2, None), self.mirror, (other, 2, None)),
        }[kind]

    def copy(self, n, kind, incoming):
        out, target, into = self.plan(kind)
        ring, shift, half = into if incoming else out
        view = self.view(n, self.block(ring, shift), half)
        return pltpu.make_async_remote_copy(
            src_ref=view,
            dst_ref=view,
            send_sem=self.send.at[n, kind],
            recv_sem=self.recv.at[n, kind],
            device_id={self.axis: target},
            device_id_type=MESH,
        )

    def start(self, n, *kinds):
        for kind in kinds:
            self.copy(n, kind, False).start()

    def arrive(self, n, *kinds):
        for kind in kinds:
            self.copy(n, kind, True).wait_recv()

    def sent(self, n, *kinds):
        for kind in kinds:
            self.copy(n, kind, False).wait_send()

    def first(self, n):
        self.start(n, 0, 1, 2)

    def second(self, n):
        self.arrive(n, 0)
        self.start(n, 3, 4)
        self.arrive(n, 1)
        self.start(n, 5)
        self.arrive(n, 2)
        self.start(n, 6)


BIAS_PIECES = 4
BIAS_KINDS = (0, 1, 2, 3, 4, 5, 6, 7, 8)
ROW_KINDS = (0, 1, 2, 3, 4, 5, 6, 9)


def row_kernel(
    x_ref, normed_ref, prior_ref, factor_ref, probe_ref, switch_ref, shift_ref, final_ref,
    mixed_ref,
    rows_ref, panel_ref, bias_ref, even_ref, odd_ref, key_ref, value_ref, query_ref, probe_t_ref,
    switch_t_ref, att_ref, max_ref,
    local_sem, row_send, row_recv, bias_send, bias_recv, pair_send, pair_recv,
):
    sequences, positions, depth = x_ref.shape
    keys = rows_ref.shape[1]
    chunks = keys // CHUNK
    res = lax.axis_index("res")
    per_piece = HEADS // BIAS_PIECES

    def row_view(n, block, half):
        size = positions if half is None else positions // 2
        low = block * positions + (0 if half is None else half * size)
        return rows_ref.at[n, pl.ds(pl.multiple_of(low, HALF), size), :]

    def bias_view(n, block, half):
        size = HALF if half is None else HALF // 2
        low = 0 if half is None else half * size
        return panel_ref.at[pl.ds(n * per_piece, per_piece), block, bias.core, pl.ds(low, size), :]

    rows = Exchange("res", 1, row_view, row_send, row_recv)
    bias = Exchange("seq", 2, bias_view, bias_send, bias_recv)
    twin = lax.axis_index("seq") + 1 - 2 * bias.core

    def pair_copy(n, core):
        view = panel_ref.at[pl.ds(n * per_piece, per_piece), :, core]
        return pltpu.make_async_remote_copy(
            src_ref=view,
            dst_ref=view,
            send_sem=pair_send.at[n],
            recv_sem=pair_recv.at[n],
            device_id={"seq": twin},
            device_id_type=MESH,
        )

    own_rows = pltpu.make_async_copy(
        normed_ref, rows_ref.at[:, pl.ds(pl.multiple_of(res * positions, positions), positions), :],
        local_sem.at[0],
    )
    own_bias = pltpu.make_async_copy(
        prior_ref, panel_ref.at[:, bias.block(bias.ring, 0), bias.core], local_sem.at[1]
    )
    own_bias.start()
    own_rows.start()

    barrier = pltpu.get_barrier_semaphore()
    peers = rows.peers() + bias.peers() + [{"seq": twin}]
    for peer in peers:
        pl.semaphore_signal(barrier, inc=1, device_id=peer, device_id_type=MESH)
    pl.semaphore_wait(barrier, len(peers))

    own_bias.wait()
    for n in range(BIAS_PIECES):
        bias.first(n)
    own_rows.wait()
    rows.first(0)
    rows.first(1)

    probe_t_ref[...] = probe_ref[0].astype(F32).T.astype(BF16)
    switch_t_ref[...] = switch_ref[0].astype(F32).T.astype(BF16)
    query_ref[...] = jnp.zeros_like(query_ref)
    scale = LOG2E / math.sqrt(WIDTH)

    @pl.loop(0, HEADS)
    def _(head):
        value_ref[head, WIDTH:, :] = jnp.ones((VROWS - WIDTH, keys), BF16)

    def bias_third(n):
        bias.arrive(n, 3)
        bias.start(n, 7)
        bias.arrive(n, 4)
        bias.start(n, 8)

    def bias_fourth(n):
        bias.arrive(n, 5, 6, 7, 8)
        pair_copy(n, bias.core).start()

    def row_third(n):
        rows.arrive(n, 5, 6)
        rows.start(n, 9)

    bias.second(0)
    rows.second(0)
    bias.second(1)
    rows.first(2)
    bias.second(2)
    rows.second(1)
    bias.second(3)
    row_third(0)
    rows.first(3)
    bias_third(0)
    bias_third(1)
    rows.second(2)
    row_third(1)
    bias_third(2)
    bias_third(3)
    rows.first(4)
    bias_fourth(0)
    bias_fourth(1)
    rows.second(3)
    row_third(2)
    bias_fourth(2)
    bias_fourth(3)
    rows.first(5)

    for n in range(BIAS_PIECES):
        pair_copy(n, 1 - bias.core).wait_recv()

        @pl.loop(n * per_piece, (n + 1) * per_piece)
        def _(head):
            @pl.loop(0, chunks)
            def _(c):
                part = panel_ref[head, c].reshape(CHUNK, positions).astype(F32)
                at = pl.ds(pl.multiple_of(c * CHUNK, CHUNK), CHUNK)
                bias_ref[head, at, :] = part * (factor_ref[head] * LOG2E)

    def scores(head, into, c):
        at = pl.ds(c * CHUNK, CHUNK)
        part = dot_nn(key_ref[head // 4, at, :], query_ref[head]) + bias_ref[head, at, :]
        into[at, :] = part
        return jnp.max(part.reshape(CHUNK // 8, 8, positions), axis=0)

    def step(head, following, source, into, top):
        total = jnp.zeros((VROWS, positions), F32)
        top_next = None
        for c in range(chunks):
            at = pl.ds(c * CHUNK, CHUNK)
            high = scores(following, into, c)
            top_next = high if top_next is None else jnp.maximum(top_next, high)
            weight = jnp.exp2(source[at, :] - top).astype(BF16)
            total = total + dot_nn(value_ref[head, :, at], weight)
        att_ref[pl.ds(pl.multiple_of(head * WIDTH, WIDTH), WIDTH), :] = (
            total[:WIDTH] / total[WIDTH : WIDTH + 1]
        )
        return jnp.max(top_next, axis=0, keepdims=True)

    @pl.loop(0, sequences)
    def _(s):
        @pl.when(s + 4 < sequences)
        def _():
            rows.second(s + 4)

        @pl.when(s + 3 < sequences)
        def _():
            row_third(s + 3)

        @pl.when(s + 6 < sequences)
        def _():
            rows.first(s + 6)

        rows.arrive(s, 3, 4, 9)
        own = rows_ref[s, pl.ds(pl.multiple_of(res * positions, positions), positions), :]

        @pl.loop(0, chunks // 4)
        def _(group):
            for k in range(4):
                at = pl.ds(pl.multiple_of(group * (4 * CHUNK) + k * CHUNK, CHUNK), CHUNK)
                part = rows_ref[s, at, :]
                key = dot_nn(part, probe_ref[1]).astype(BF16)
                key_ref[0, at, :] = key[:, :HALF]
                key_ref[1, at, :] = key[:, HALF:]
                value = dot_nt(switch_t_ref[...], part).astype(BF16)
                for head in range(HEADS):
                    value_ref[head, :WIDTH, at] = value[head * WIDTH : (head + 1) * WIDTH]

        query = (dot_nt(probe_t_ref[...], own) * scale).astype(BF16)
        for head in range(HEADS):
            low = head % 4 * WIDTH
            query_ref[head, low : low + WIDTH, :] = query[head * WIDTH : (head + 1) * WIDTH]
        top = scores(0, even_ref, 0)
        for c in range(1, chunks):
            top = jnp.maximum(top, scores(0, even_ref, c))
        max_ref[...] = jnp.max(top, axis=0, keepdims=True)

        @pl.loop(0, HEADS // 2)
        def _(pair):
            head = pair * 2
            top = step(head, head + 1, even_ref, odd_ref, max_ref[...])
            max_ref[...] = step(head + 1, lax.rem(head + 2, HEADS), odd_ref, even_ref, top)

        gates = jax.nn.sigmoid(dot_nn(own, switch_ref[1]) + shift_ref[...])
        attended = (att_ref[...].T * gates).astype(BF16)
        mixed_ref[s] = x_ref[s].astype(F32) + dot_nn(attended, final_ref[...])


    @pl.loop(0, sequences)
    def _(n):
        rows.sent(n, *ROW_KINDS)

    @pl.loop(0, BIAS_PIECES)
    def _(n):
        bias.sent(n, *BIAS_KINDS)
        pair_copy(n, bias.core).wait_send()


def row_attention(x, normed, prior, factor, probe, switch, shift, final):
    sequences, positions, depth = x.shape
    keys = positions * lax.axis_size("res")
    chips = lax.axis_size("seq") // 2
    vmem = pl.BlockSpec(memory_space=VM)
    hbm = pl.BlockSpec(memory_space=pl.ANY)
    dma = pltpu.SemaphoreType.DMA
    return pl.pallas_call(
        row_kernel,
        out_shape=jax.ShapeDtypeStruct(x.shape, F32),
        in_specs=[vmem, hbm, hbm, pl.BlockSpec(memory_space=pltpu.SMEM)] + [vmem] * 4,
        out_specs=vmem,
        scratch_shapes=[
            VM((sequences, keys, depth), BF16),
            VM((HEADS, chips, 2, HALF, positions), BF16),
            VM((HEADS, keys, positions), F32),
            VM((keys, positions), F32),
            VM((keys, positions), F32),
            VM((2, keys, HALF), BF16),
            VM((HEADS, VROWS, keys), BF16),
            VM((HEADS, HALF, positions), BF16),
            VM((depth, depth), BF16),
            VM((depth, depth), BF16),
            VM((depth, positions), F32),
            VM((1, positions), F32),
            dma((2,)),
            dma((sequences, 10)),
            dma((sequences, 10)),
            dma((BIAS_PIECES, 9)),
            dma((BIAS_PIECES, 9)),
            dma((BIAS_PIECES,)),
            dma((BIAS_PIECES,)),
        ],
        compiler_params=pltpu.CompilerParams(
            vmem_limit_bytes=66_000_000, collective_id=0, has_side_effects=True
        ),
    )(x, normed, prior, factor, probe, switch, shift[None], final)


def column_kernel(
    rows_ref, norm_ref, probe_ref, switch_ref, shift_ref, final_ref,
    out_ref,
    left_ref, right_ref, probe_t_ref, switch_t_ref, query_ref, att_ref,
):
    count, residues, depth = rows_ref.shape
    probe_t_ref[...] = probe_ref[0].astype(F32).T.astype(BF16)
    switch_t_ref[...] = switch_ref[0].astype(F32).T.astype(BF16)
    query_ref[...] = jnp.zeros_like(query_ref)
    scale = LOG2E / math.sqrt(WIDTH)
    step = 16

    @pl.loop(0, count // step)
    def _(i):
        part = rows_ref[pl.ds(pl.multiple_of(i * step, step), step)].astype(F32)
        part = part.reshape(step * residues, depth)
        rows = step * residues
        part = standardize(part, norm_ref[...])
        at = pl.ds(pl.multiple_of(i * rows, rows), rows)
        left_ref[at, :] = part[:, :HALF]
        right_ref[at, :] = part[:, HALF:]

    @pl.loop(0, residues)
    def _(r):
        spots = pl.ds(r, count, stride=residues)
        normed = jnp.concatenate([left_ref[spots, :], right_ref[spots, :]], axis=1).astype(BF16)
        key = dot_nn(normed, probe_ref[1]).astype(BF16)
        query = (dot_nt(probe_t_ref[...], normed) * scale).astype(BF16)
        value = dot_nt(switch_t_ref[...], normed).astype(BF16)
        gates = jax.nn.sigmoid(dot_nn(normed, switch_ref[1]) + shift_ref[...])
        ones = jnp.ones((16, count), BF16)
        for half in range(2):
            for k in range(4):
                low = k * WIDTH
                query_ref[low : low + WIDTH, k * count : (k + 1) * count] = query[
                    half * HALF + low : half * HALF + low + WIDTH
                ]
            score = dot_nn(key[:, half * HALF : (half + 1) * HALF], query_ref[...])
            top = jnp.max(score, axis=0, keepdims=True)
            weight = jnp.exp2(score - top).astype(BF16)
            for k in range(4):
                low = half * HALF + k * WIDTH
                block = jnp.concatenate([value[low : low + WIDTH], ones], axis=0)
                total = dot_nn(block, weight[:, k * count : (k + 1) * count])
                att_ref[low : low + WIDTH, :] = total[:WIDTH] / total[WIDTH : WIDTH + 1]
        attended = (att_ref[...].T * gates).astype(BF16)
        delta = dot_nn(attended, final_ref[...])
        left_ref[spots, :] = delta[:, :HALF]
        right_ref[spots, :] = delta[:, HALF:]

    @pl.loop(0, count // step)
    def _(i):
        rows = step * residues
        at = pl.ds(pl.multiple_of(i * rows, rows), rows)
        part = jnp.concatenate([left_ref[at, :], right_ref[at, :]], axis=1)
        out_ref[pl.ds(pl.multiple_of(i * step, step), step)] = part.astype(BF16).reshape(
            step, residues, depth
        )


def column_attention(rows, norm, probe, switch, shift, final):
    count, residues, depth = rows.shape
    vmem = pl.BlockSpec(memory_space=VM)
    return pl.pallas_call(
        column_kernel,
        out_shape=jax.ShapeDtypeStruct(rows.shape, BF16),
        in_specs=[vmem] * 6,
        out_specs=vmem,
        scratch_shapes=[
            VM((count * residues, HALF), F32),
            VM((count * residues, HALF), F32),
            VM((depth, depth), BF16),
            VM((depth, depth), BF16),
            VM((HALF, 4 * count), BF16),
            VM((depth, count), F32),
        ],
    )(rows, norm[None], probe, switch, shift[None], final)


def standardize_features(row_data, standardize_factor):
    row_data = row_data.astype(F32)
    row_mean = jnp.mean(row_data, -1, keepdims=True)
    centred = row_data - row_mean
    deviation = jnp.mean(centred * centred, -1, keepdims=True)
    return (centred * lax.rsqrt(deviation + EPS) * standardize_factor).astype(BF16)


def shards(x, prior, factor, norm_h, probe_h, switch_h, shift_h, final_h, norm_v, probe_v, switch_v, shift_v, final_v):
    sequences, positions, depth = x.shape
    normed = standardize_features(x, norm_h)
    mixed = row_attention(x, normed, prior.transpose(0, 2, 1), factor, probe_h, switch_h, shift_h, final_h)
    seq_count = lax.axis_size("seq")
    slices = positions // seq_count
    layered = mixed.astype(BF16).reshape(sequences, seq_count, slices, depth)
    columns = lax.all_to_all(layered, "seq", split_axis=1, concat_axis=0, tiled=True)
    delta = column_attention(columns[:, 0], norm_v, probe_v, switch_v, shift_v, final_v)
    back = lax.all_to_all(delta[:, None], "seq", split_axis=0, concat_axis=1, tiled=True)
    return mixed + back.reshape(sequences, positions, depth).astype(F32)


def solution(mesh):
    placed = (P("seq", "res", None), P(None, "res", "seq")) + (P(),) * 11
    return jax.shard_map(
        shards, mesh=mesh, in_specs=placed, out_specs=P("seq", "res", None), check_vma=False
    )
```

```python
import functools
import math

import jax
import jax.numpy as jnp
from jax import lax
from jax.experimental import pallas as pl
from jax.experimental.pallas import tpu as pltpu
from jax.sharding import PartitionSpec as P

EPS = 1e-05
LOG2E = 1.4426950408889634
F32 = jnp.float32
BF16 = jnp.bfloat16
HEADS = 8
WIDTH = 32
HALF = 128
VROWS = 48
CHUNK = 256
VM = pltpu.VMEM


def dot_nn(a, b):
    return lax.dot_general(a, b, (((1,), (0,)), ((), ())), preferred_element_type=F32)


def dot_nt(a, b):
    return lax.dot_general(a, b, (((1,), (1,)), ((), ())), preferred_element_type=F32)


def standardize(x, factor):
    mean = jnp.sum(x, -1, keepdims=True) * (1.0 / x.shape[-1])
    centred = x - mean
    var = jnp.sum(centred * centred, -1, keepdims=True) * (1.0 / x.shape[-1])
    return centred * lax.rsqrt(var + EPS) * factor


MESH = pl.DeviceIdType.MESH
RING = 4


class Exchange:
    def __init__(self, axis, cores, view, send, recv):
        index = lax.axis_index(axis)
        self.axis, self.cores, self.view, self.send, self.recv = axis, cores, view, send, recv
        self.core = lax.rem(index, cores)
        chip = index // cores
        self.ring, self.at = chip // RING, lax.rem(chip, RING)
        self.mirror = self.device(1 - self.ring, 0)
        self.up, self.down = self.device(self.ring, 1), self.device(self.ring, -1)

    def block(self, ring, shift):
        return ring * RING + lax.rem(self.at + (shift + RING), RING)

    def device(self, ring, shift):
        return self.block(ring, shift) * self.cores + self.core

    def peers(self):
        return [{self.axis: d} for d in (self.mirror, self.up, self.down)]

    def plan(self, kind):
        mine, other = self.ring, 1 - self.ring
        return {
            0: ((mine, 0, None), self.mirror, (other, 0, None)),
            1: ((mine, 0, None), self.up, (mine, -1, None)),
            2: ((mine, 0, None), self.down, (mine, 1, None)),
            3: ((other, 0, None), self.up, (other, -1, None)),
            4: ((other, 0, None), self.down, (other, 1, None)),
            5: ((mine, -1, 0), self.up, (mine, -2, 0)),
            6: ((mine, 1, 1), self.down, (mine, 2, 1)),
            7: ((other, -1, 0), self.up, (other, -2, 0)),
            8: ((other, 1, 1), self.down, (other, 2, 1)),
            9: ((mine, 2, None), self.mirror, (other, 2, None)),
        }[kind]

    def copy(self, n, kind, incoming):
        out, target, into = self.plan(kind)
        ring, shift, half = into if incoming else out
        view = self.view(n, self.block(ring, shift), half)
        return pltpu.make_async_remote_copy(
            src_ref=view,
            dst_ref=view,
            send_sem=self.send.at[n, kind],
            recv_sem=self.recv.at[n, kind],
            device_id={self.axis: target},
            device_id_type=MESH,
        )

    def start(self, n, *kinds):
        for kind in kinds:
            self.copy(n, kind, False).start()

    def arrive(self, n, *kinds):
        for kind in kinds:
            self.copy(n, kind, True).wait_recv()

    def sent(self, n, *kinds):
        for kind in kinds:
            self.copy(n, kind, False).wait_send()

    def first(self, n):
        self.start(n, 0, 1, 2)

    def second(self, n):
        self.arrive(n, 0)
        self.start(n, 3, 4)
        self.arrive(n, 1)
        self.start(n, 5)
        self.arrive(n, 2)
        self.start(n, 6)


BIAS_PIECES = 4
BIAS_KINDS = (0, 1, 2, 3, 4, 5, 6, 7, 8)
ROW_KINDS = (0, 1, 2, 3, 4, 5, 6, 9)


def row_kernel(
    x_ref, prior_ref, factor_ref, norm_ref, probe_ref, switch_ref, shift_ref, final_ref,
    mixed_ref, columns_ref,
    stage_ref, rows_ref, panel_ref, bias_ref, even_ref, odd_ref, key_ref, value_ref, query_ref, probe_t_ref,
    switch_t_ref, att_ref, max_ref,
    row_send, row_recv, bias_send, bias_recv, pair_send, pair_recv, column_send, column_recv,
):
    sequences, positions, depth = x_ref.shape
    keys = rows_ref.shape[1]
    chunks = keys // CHUNK
    res = lax.axis_index("res")
    per_piece = HEADS // BIAS_PIECES

    def row_view(n, block, half):
        size = positions if half is None else positions // 2
        low = block * positions + (0 if half is None else half * size)
        return rows_ref.at[n, pl.ds(pl.multiple_of(low, HALF), size), :]

    def bias_view(n, block, half):
        size = HALF if half is None else HALF // 2
        low = 0 if half is None else half * size
        return panel_ref.at[pl.ds(n * per_piece, per_piece), block, bias.core, pl.ds(low, size), :]

    rows = Exchange("res", 1, row_view, row_send, row_recv)
    bias = Exchange("seq", 2, bias_view, bias_send, bias_recv)
    twin = lax.axis_index("seq") + 1 - 2 * bias.core

    def pair_copy(n, core):
        view = panel_ref.at[pl.ds(n * per_piece, per_piece), :, core]
        return pltpu.make_async_remote_copy(
            src_ref=view,
            dst_ref=view,
            send_sem=pair_send.at[n],
            recv_sem=pair_recv.at[n],
            device_id={"seq": twin},
            device_id_type=MESH,
        )

    seq = lax.axis_index("seq")
    seq_count = columns_ref.shape[0] // sequences
    residues = columns_ref.shape[1]

    def column_copy(n, target):
        return pltpu.make_async_remote_copy(
            src_ref=stage_ref.at[n, pl.ds(pl.multiple_of(target * residues, residues), residues), :],
            dst_ref=columns_ref.at[seq * sequences + n],
            send_sem=column_send,
            recv_sem=column_recv,
            device_id={"seq": target},
            device_id_type=MESH,
        )

    def send_columns(n):
        @pl.loop(1, seq_count)
        def _(k):
            column_copy(n, lax.rem(seq + k, seq_count)).start()

    barrier = pltpu.get_barrier_semaphore()
    for peer in rows.peers():
        pl.semaphore_signal(barrier, inc=1, device_id=peer, device_id_type=MESH)

    @pl.loop(1, seq_count)
    def _(k):
        peer = {"seq": lax.rem(seq + k, seq_count)}
        pl.semaphore_signal(barrier, inc=1, device_id=peer, device_id_type=MESH)

    for head in range(HEADS):
        panel_ref[head, bias.block(bias.ring, 0), bias.core] = (
            prior_ref[head].astype(F32).T.astype(BF16)
        )

    own_spot = pl.ds(pl.multiple_of(res * positions, positions), positions)

    @pl.loop(0, sequences)
    def _(s):
        rows_ref[s, own_spot, :] = standardize(x_ref[s].astype(F32), norm_ref[...]).astype(BF16)

    pl.semaphore_wait(barrier, 3 + seq_count - 1)
    for n in range(BIAS_PIECES):
        bias.first(n)
    rows.first(0)
    rows.first(1)

    probe_t_ref[...] = probe_ref[0].astype(F32).T.astype(BF16)
    switch_t_ref[...] = switch_ref[0].astype(F32).T.astype(BF16)
    query_ref[...] = jnp.zeros_like(query_ref)
    scale = LOG2E / math.sqrt(WIDTH)

    @pl.loop(0, HEADS)
    def _(head):
        value_ref[head, WIDTH:, :] = jnp.ones((VROWS - WIDTH, keys), BF16)

    def bias_third(n):
        bias.arrive(n, 3)
        bias.start(n, 7)
        bias.arrive(n, 4)
        bias.start(n, 8)

    def bias_fourth(n):
        bias.arrive(n, 5, 6, 7, 8)
        pair_copy(n, bias.core).start()

    def row_third(n):
        rows.arrive(n, 5, 6)
        rows.start(n, 9)

    bias.second(0)
    rows.second(0)
    bias.second(1)
    rows.first(2)
    bias.second(2)
    rows.second(1)
    bias.second(3)
    row_third(0)
    rows.first(3)
    bias_third(0)
    bias_third(1)
    rows.second(2)
    row_third(1)
    bias_third(2)
    bias_third(3)
    rows.first(4)
    bias_fourth(0)
    bias_fourth(1)
    rows.second(3)
    row_third(2)
    bias_fourth(2)
    bias_fourth(3)
    rows.first(5)

    for n in range(BIAS_PIECES):
        pair_copy(n, 1 - bias.core).wait_recv()

        @pl.loop(n * per_piece, (n + 1) * per_piece)
        def _(head):
            @pl.loop(0, chunks)
            def _(c):
                part = panel_ref[head, c].reshape(CHUNK, positions).astype(F32)
                at = pl.ds(pl.multiple_of(c * CHUNK, CHUNK), CHUNK)
                bias_ref[head, at, :] = part * (factor_ref[head] * LOG2E)

    def scores(head, into, c):
        at = pl.ds(c * CHUNK, CHUNK)
        part = dot_nn(key_ref[head // 4, at, :], query_ref[head]) + bias_ref[head, at, :]
        into[at, :] = part
        return jnp.max(part.reshape(CHUNK // 8, 8, positions), axis=0)

    def step(head, following, source, into, top):
        total = jnp.zeros((VROWS, positions), F32)
        top_next = None
        for c in range(chunks):
            at = pl.ds(c * CHUNK, CHUNK)
            high = scores(following, into, c)
            top_next = high if top_next is None else jnp.maximum(top_next, high)
            weight = jnp.exp2(source[at, :] - top).astype(BF16)
            total = total + dot_nn(value_ref[head, :, at], weight)
        att_ref[pl.ds(pl.multiple_of(head * WIDTH, WIDTH), WIDTH), :] = (
            total[:WIDTH] / total[WIDTH : WIDTH + 1]
        )
        return jnp.max(top_next, axis=0, keepdims=True)

    @pl.loop(0, sequences)
    def _(s):
        @pl.when(s + 4 < sequences)
        def _():
            rows.second(s + 4)

        @pl.when(s + 3 < sequences)
        def _():
            row_third(s + 3)

        @pl.when(s + 6 < sequences)
        def _():
            rows.first(s + 6)

        @pl.when(s > 0)
        def _():
            send_columns(s - 1)

        rows.arrive(s, 3, 4, 9)
        own = rows_ref[s, own_spot, :]

        @pl.loop(0, chunks // 4)
        def _(group):
            for k in range(4):
                at = pl.ds(pl.multiple_of(group * (4 * CHUNK) + k * CHUNK, CHUNK), CHUNK)
                part = rows_ref[s, at, :]
                key = dot_nn(part, probe_ref[1]).astype(BF16)
                key_ref[0, at, :] = key[:, :HALF]
                key_ref[1, at, :] = key[:, HALF:]
                value = dot_nt(switch_t_ref[...], part).astype(BF16)
                for head in range(HEADS):
                    value_ref[head, :WIDTH, at] = value[head * WIDTH : (head + 1) * WIDTH]

        query = (dot_nt(probe_t_ref[...], own) * scale).astype(BF16)
        for head in range(HEADS):
            low = head % 4 * WIDTH
            query_ref[head, low : low + WIDTH, :] = query[head * WIDTH : (head + 1) * WIDTH]
        top = scores(0, even_ref, 0)
        for c in range(1, chunks):
            top = jnp.maximum(top, scores(0, even_ref, c))
        max_ref[...] = jnp.max(top, axis=0, keepdims=True)

        @pl.loop(0, HEADS // 2)
        def _(pair):
            head = pair * 2
            top = step(head, head + 1, even_ref, odd_ref, max_ref[...])
            max_ref[...] = step(head + 1, lax.rem(head + 2, HEADS), odd_ref, even_ref, top)

        gates = jax.nn.sigmoid(dot_nn(own, switch_ref[1]) + shift_ref[...])
        attended = (att_ref[...].T * gates).astype(BF16)
        mixed = x_ref[s].astype(F32) + dot_nn(attended, final_ref[...])
        mixed_ref[s] = mixed
        stage_ref[s] = mixed.astype(BF16)
        columns_ref[seq * sequences + s] = stage_ref[
            s, pl.ds(pl.multiple_of(seq * residues, residues), residues), :
        ]


    send_columns(sequences - 1)

    @pl.loop(0, sequences)
    def _(n):
        rows.sent(n, *ROW_KINDS)

    @pl.loop(0, BIAS_PIECES)
    def _(n):
        bias.sent(n, *BIAS_KINDS)
        pair_copy(n, bias.core).wait_send()

    moved = columns_ref.at[pl.ds(0, sequences * (seq_count - 1))]
    every = pltpu.make_async_remote_copy(
        src_ref=moved,
        dst_ref=moved,
        send_sem=column_send,
        recv_sem=column_recv,
        device_id={"seq": twin},
        device_id_type=MESH,
    )
    every.wait_send()
    every.wait_recv()


def row_attention(x, prior, factor, norm, probe, switch, shift, final):
    sequences, positions, depth = x.shape
    keys = positions * lax.axis_size("res")
    seq_count = lax.axis_size("seq")
    vmem = pl.BlockSpec(memory_space=VM)
    dma = pltpu.SemaphoreType.DMA
    return pl.pallas_call(
        row_kernel,
        out_shape=[
            jax.ShapeDtypeStruct(x.shape, F32),
            jax.ShapeDtypeStruct((sequences * seq_count, positions // seq_count, depth), BF16),
        ],
        in_specs=[vmem, vmem, pl.BlockSpec(memory_space=pltpu.SMEM)] + [vmem] * 5,
        out_specs=[vmem, vmem],
        scratch_shapes=[
            VM((sequences, positions, depth), BF16),
            VM((sequences, keys, depth), BF16),
            VM((HEADS, seq_count // 2, 2, HALF, positions), BF16),
            VM((HEADS, keys, positions), F32),
            VM((keys, positions), F32),
            VM((keys, positions), F32),
            VM((2, keys, HALF), BF16),
            VM((HEADS, VROWS, keys), BF16),
            VM((HEADS, HALF, positions), BF16),
            VM((depth, depth), BF16),
            VM((depth, depth), BF16),
            VM((depth, positions), F32),
            VM((1, positions), F32),
            dma((sequences, 10)),
            dma((sequences, 10)),
            dma((BIAS_PIECES, 9)),
            dma((BIAS_PIECES, 9)),
            dma((BIAS_PIECES,)),
            dma((BIAS_PIECES,)),
            dma,
            dma,
        ],
        compiler_params=pltpu.CompilerParams(
            vmem_limit_bytes=66_000_000, collective_id=0, has_side_effects=True
        ),
    )(x, prior, factor, norm[None], probe, switch, shift[None], final)


def column_kernel(
    rows_ref, norm_ref, probe_ref, switch_ref, shift_ref, final_ref,
    back_ref,
    left_ref, right_ref, out_left_ref, out_right_ref, stage_ref, probe_t_ref, switch_t_ref,
    query_ref, att_ref,
    send_sem, recv_sem,
):
    count, residues, depth = rows_ref.shape
    seq = lax.axis_index("seq")
    seq_count = lax.axis_size("seq")
    sequences = back_ref.shape[0]
    part_size = stage_ref.shape[2]
    barrier = pltpu.get_barrier_semaphore()

    @pl.loop(1, seq_count)
    def _(k):
        peer = {"seq": lax.rem(seq + k, seq_count)}
        pl.semaphore_signal(barrier, inc=1, device_id=peer, device_id_type=MESH)

    probe_t_ref[...] = probe_ref[0].astype(F32).T.astype(BF16)
    switch_t_ref[...] = switch_ref[0].astype(F32).T.astype(BF16)
    query_ref[...] = jnp.zeros_like(query_ref)
    scale = LOG2E / math.sqrt(WIDTH)
    step = 16

    @pl.loop(0, count // step)
    def _(i):
        part = rows_ref[pl.ds(pl.multiple_of(i * step, step), step)].astype(F32)
        rows = step * residues
        part = standardize(part.reshape(rows, depth), norm_ref[...])
        at = pl.ds(pl.multiple_of(i * rows, rows), rows)
        left_ref[at, :] = part[:, :HALF]
        right_ref[at, :] = part[:, HALF:]

    ones = jnp.ones((16, count), BF16)

    def attend(r, slot):
        normed = jnp.concatenate(
            [
                jnp.concatenate(
                    [
                        left_ref[pl.ds(r + k, count, stride=residues), :],
                        right_ref[pl.ds(r + k, count, stride=residues), :],
                    ],
                    axis=1,
                )
                for k in range(2)
            ],
            axis=0,
        ).astype(BF16)
        key = dot_nn(normed, probe_ref[1]).astype(BF16)
        query = (dot_nt(probe_t_ref[...], normed) * scale).astype(BF16)
        value = dot_nt(switch_t_ref[...], normed).astype(BF16)
        gates = jax.nn.sigmoid(dot_nn(normed, switch_ref[1]) + shift_ref[...])
        for k in range(2):
            mine = slice(k * count, (k + 1) * count)
            for half in range(2):
                spot = 4 * slot + 2 * k + half
                for h in range(4):
                    low = h * WIDTH
                    query_ref[spot, low : low + WIDTH, h * count : (h + 1) * count] = query[
                        half * HALF + low : half * HALF + low + WIDTH, mine
                    ]
                score = dot_nn(key[mine, half * HALF : (half + 1) * HALF], query_ref[spot])
                top = jnp.max(score, axis=0, keepdims=True)
                weight = jnp.exp2(score - top).astype(BF16)
                for h in range(0, 4, 2):
                    low = half * HALF + h * WIDTH
                    block = jnp.concatenate([value[low : low + 2 * WIDTH, mine], ones], axis=0)
                    total = dot_nn(block, weight[:, h * count : (h + 2) * count])
                    for j in range(2):
                        spread = slice(j * count, (j + 1) * count)
                        att_ref[
                            slot, low + j * WIDTH : low + (j + 1) * WIDTH, k * count : (k + 1) * count
                        ] = (
                            total[j * WIDTH : (j + 1) * WIDTH, spread]
                            / total[2 * WIDTH : 2 * WIDTH + 1, spread]
                        )
        attended = (att_ref[slot].T * gates).astype(BF16)
        return dot_nn(attended, final_ref[...])

    def back_copy(part, target):
        return pltpu.make_async_remote_copy(
            src_ref=stage_ref.at[part, pl.ds(target * sequences, sequences)],
            dst_ref=back_ref.at[
                :, pl.ds(pl.multiple_of(seq * residues + part * part_size, part_size), part_size), :
            ],
            send_sem=send_sem,
            recv_sem=recv_sem,
            device_id={"seq": target},
            device_id_type=MESH,
        )

    pairs = 2
    for part in range(residues // part_size):

        @pl.loop(0, part_size // (2 * pairs))
        def _(group):
            low = group * (2 * pairs)
            deltas = [attend(part * part_size + low + 2 * p, p) for p in range(pairs)]
            for p, delta in enumerate(deltas):
                for k in range(2):
                    spots = pl.ds(low + 2 * p + k, count, stride=part_size)
                    out_left_ref[spots, :] = delta[k * count : (k + 1) * count, :HALF]
                    out_right_ref[spots, :] = delta[k * count : (k + 1) * count, HALF:]

        @pl.loop(0, count // step)
        def _(i):
            rows = step * part_size
            at = pl.ds(pl.multiple_of(i * rows, rows), rows)
            block = jnp.concatenate([out_left_ref[at, :], out_right_ref[at, :]], axis=1)
            stage_ref[part, pl.ds(pl.multiple_of(i * step, step), step)] = block.astype(BF16).reshape(
                step, part_size, depth
            )

        if part == 0:
            pl.semaphore_wait(barrier, seq_count - 1)

        @pl.loop(1, seq_count)
        def _(k):
            back_copy(part, lax.rem(seq + k, seq_count)).start()

        back_ref[
            :, pl.ds(pl.multiple_of(seq * residues + part * part_size, part_size), part_size), :
        ] = stage_ref[part, pl.ds(seq * sequences, sequences)]

    moved = back_ref.at[:, pl.ds(0, residues * (seq_count - 1)), :]
    every = pltpu.make_async_remote_copy(
        src_ref=moved,
        dst_ref=moved,
        send_sem=send_sem,
        recv_sem=recv_sem,
        device_id={"seq": lax.rem(seq + 1, seq_count)},
        device_id_type=MESH,
    )
    every.wait_send()
    every.wait_recv()


def column_attention(rows, norm, probe, switch, shift, final):
    count, residues, depth = rows.shape
    seq_count = lax.axis_size("seq")
    part_size = residues // 2
    vmem = pl.BlockSpec(memory_space=VM)
    dma = pltpu.SemaphoreType.DMA
    return pl.pallas_call(
        column_kernel,
        out_shape=jax.ShapeDtypeStruct((count // seq_count, residues * seq_count, depth), BF16),
        in_specs=[vmem] * 6,
        out_specs=vmem,
        scratch_shapes=[
            VM((count * residues, HALF), F32),
            VM((count * residues, HALF), F32),
            VM((count * part_size, HALF), F32),
            VM((count * part_size, HALF), F32),
            VM((residues // part_size, count, part_size, depth), BF16),
            VM((depth, depth), BF16),
            VM((depth, depth), BF16),
            VM((8, HALF, 4 * count), BF16),
            VM((2, depth, 2 * count), F32),
            dma,
            dma,
        ],
        compiler_params=pltpu.CompilerParams(collective_id=1, has_side_effects=True),
    )(rows, norm[None], probe, switch, shift[None], final)


def shards(x, prior, factor, norm_h, probe_h, switch_h, shift_h, final_h, norm_v, probe_v, switch_v, shift_v, final_v):
    mixed, columns = row_attention(x, prior, factor, norm_h, probe_h, switch_h, shift_h, final_h)
    back = column_attention(columns, norm_v, probe_v, switch_v, shift_v, final_v)
    return mixed + back.astype(F32)


def solution(mesh):
    placed = (P("seq", "res", None), P(None, "res", "seq")) + (P(),) * 11
    return jax.shard_map(
        shards, mesh=mesh, in_specs=placed, out_specs=P("seq", "res", None), check_vma=False
    )
```

```python
import functools
import math

import jax
import jax.numpy as jnp
from jax import lax
from jax.experimental import pallas as pl
from jax.experimental.pallas import tpu as pltpu
from jax.sharding import PartitionSpec as P

EPS = 1e-05
LOG2E = 1.4426950408889634
F32 = jnp.float32
BF16 = jnp.bfloat16
HEADS = 8
WIDTH = 32
HALF = 128
VROWS = 48
CHUNK = 256
VM = pltpu.VMEM


def dot_nn(a, b):
    return lax.dot_general(a, b, (((1,), (0,)), ((), ())), preferred_element_type=F32)


def dot_nt(a, b):
    return lax.dot_general(a, b, (((1,), (1,)), ((), ())), preferred_element_type=F32)


def standardize(x, factor):
    mean = jnp.sum(x, -1, keepdims=True) * (1.0 / x.shape[-1])
    centred = x - mean
    var = jnp.sum(centred * centred, -1, keepdims=True) * (1.0 / x.shape[-1])
    return centred * lax.rsqrt(var + EPS) * factor


MESH = pl.DeviceIdType.MESH
RING = 4


class Exchange:
    def __init__(self, axis, cores, view, send, recv):
        index = lax.axis_index(axis)
        self.axis, self.cores, self.view, self.send, self.recv = axis, cores, view, send, recv
        self.core = lax.rem(index, cores)
        chip = index // cores
        self.ring, self.at = chip // RING, lax.rem(chip, RING)
        self.mirror = self.device(1 - self.ring, 0)
        self.up, self.down = self.device(self.ring, 1), self.device(self.ring, -1)

    def block(self, ring, shift):
        return ring * RING + lax.rem(self.at + (shift + RING), RING)

    def device(self, ring, shift):
        return self.block(ring, shift) * self.cores + self.core

    def peers(self):
        return [{self.axis: d} for d in (self.mirror, self.up, self.down)]

    def plan(self, kind):
        mine, other = self.ring, 1 - self.ring
        return {
            0: ((mine, 0, None), self.mirror, (other, 0, None)),
            1: ((mine, 0, None), self.up, (mine, -1, None)),
            2: ((mine, 0, None), self.down, (mine, 1, None)),
            3: ((other, 0, None), self.up, (other, -1, None)),
            4: ((other, 0, None), self.down, (other, 1, None)),
            5: ((mine, -1, 0), self.up, (mine, -2, 0)),
            6: ((mine, 1, 1), self.down, (mine, 2, 1)),
            7: ((other, -1, 0), self.up, (other, -2, 0)),
            8: ((other, 1, 1), self.down, (other, 2, 1)),
            9: ((mine, 2, None), self.mirror, (other, 2, None)),
        }[kind]

    def copy(self, n, kind, incoming):
        out, target, into = self.plan(kind)
        ring, shift, half = into if incoming else out
        view = self.view(n, self.block(ring, shift), half)
        return pltpu.make_async_remote_copy(
            src_ref=view,
            dst_ref=view,
            send_sem=self.send.at[n, kind],
            recv_sem=self.recv.at[n, kind],
            device_id={self.axis: target},
            device_id_type=MESH,
        )

    def start(self, n, *kinds):
        for kind in kinds:
            self.copy(n, kind, False).start()

    def arrive(self, n, *kinds):
        for kind in kinds:
            self.copy(n, kind, True).wait_recv()

    def sent(self, n, *kinds):
        for kind in kinds:
            self.copy(n, kind, False).wait_send()

    def first(self, n):
        self.start(n, 0, 1, 2)

    def second(self, n):
        self.arrive(n, 0)
        self.start(n, 3, 4)
        self.arrive(n, 1)
        self.start(n, 5)
        self.arrive(n, 2)
        self.start(n, 6)


BIAS_PIECES = 4
BIAS_KINDS = (0, 1, 2, 3, 4, 5, 6, 7, 8)
ROW_KINDS = (0, 1, 2, 3, 4, 5, 6, 9)


def row_kernel(
    x_ref, prior_ref, factor_ref, norm_ref, probe_ref, switch_ref, shift_ref, final_ref,
    mixed_ref, columns_ref,
    stage_ref, rows_ref, panel_ref, bias_ref, even_ref, odd_ref, key_ref, value_ref, query_ref, probe_t_ref,
    switch_t_ref, att_ref, max_ref,
    row_send, row_recv, bias_send, bias_recv, pair_send, pair_recv, column_send, column_recv,
):
    sequences, positions, depth = x_ref.shape
    keys = rows_ref.shape[1]
    chunks = keys // CHUNK
    res = lax.axis_index("res")
    per_piece = HEADS // BIAS_PIECES

    def row_view(n, block, half):
        size = positions if half is None else positions // 2
        low = block * positions + (0 if half is None else half * size)
        return rows_ref.at[n, pl.ds(pl.multiple_of(low, HALF), size), :]

    def bias_view(n, block, half):
        size = HALF if half is None else HALF // 2
        low = 0 if half is None else half * size
        return panel_ref.at[pl.ds(n * per_piece, per_piece), block, bias.core, pl.ds(low, size), :]

    rows = Exchange("res", 1, row_view, row_send, row_recv)
    bias = Exchange("seq", 2, bias_view, bias_send, bias_recv)
    twin = lax.axis_index("seq") + 1 - 2 * bias.core

    def pair_copy(n, core):
        view = panel_ref.at[pl.ds(n * per_piece, per_piece), :, core]
        return pltpu.make_async_remote_copy(
            src_ref=view,
            dst_ref=view,
            send_sem=pair_send.at[n],
            recv_sem=pair_recv.at[n],
            device_id={"seq": twin},
            device_id_type=MESH,
        )

    seq = lax.axis_index("seq")
    seq_count = columns_ref.shape[0] // sequences
    residues = columns_ref.shape[1]

    def column_copy(n, target):
        return pltpu.make_async_remote_copy(
            src_ref=stage_ref.at[n, pl.ds(pl.multiple_of(target * residues, residues), residues), :],
            dst_ref=columns_ref.at[seq * sequences + n],
            send_sem=column_send,
            recv_sem=column_recv,
            device_id={"seq": target},
            device_id_type=MESH,
        )

    def send_columns(n):
        @pl.loop(1, seq_count)
        def _(k):
            column_copy(n, lax.rem(seq + k, seq_count)).start()

    barrier = pltpu.get_barrier_semaphore()
    for peer in rows.peers():
        pl.semaphore_signal(barrier, inc=1, device_id=peer, device_id_type=MESH)

    @pl.loop(1, seq_count)
    def _(k):
        peer = {"seq": lax.rem(seq + k, seq_count)}
        pl.semaphore_signal(barrier, inc=1, device_id=peer, device_id_type=MESH)

    for head in range(HEADS):
        panel_ref[head, bias.block(bias.ring, 0), bias.core] = (
            prior_ref[head].astype(F32).T.astype(BF16)
        )

    own_spot = pl.ds(pl.multiple_of(res * positions, positions), positions)

    @pl.loop(0, sequences)
    def _(s):
        rows_ref[s, own_spot, :] = standardize(x_ref[s].astype(F32), norm_ref[...]).astype(BF16)

    pl.semaphore_wait(barrier, 3 + seq_count - 1)
    for n in range(BIAS_PIECES):
        bias.first(n)
    for n in range(sequences):
        rows.first(n)

    probe_t_ref[...] = probe_ref[0].astype(F32).T.astype(BF16)
    switch_t_ref[...] = switch_ref[0].astype(F32).T.astype(BF16)
    query_ref[...] = jnp.zeros_like(query_ref)
    scale = LOG2E / math.sqrt(WIDTH)

    @pl.loop(0, 2 * HEADS)
    def _(spot):
        value_ref[spot, WIDTH:, :] = jnp.ones((VROWS - WIDTH, keys), BF16)

    def bias_third(n):
        bias.arrive(n, 3)
        bias.start(n, 7)
        bias.arrive(n, 4)
        bias.start(n, 8)

    def bias_fourth(n):
        bias.arrive(n, 5, 6, 7, 8)
        pair_copy(n, bias.core).start()

    def bias_done(n):
        pair_copy(n, 1 - bias.core).wait_recv()

        @pl.loop(0, per_piece * chunks)
        def _(k):
            head = n * per_piece + k // chunks
            c = lax.rem(k, chunks)
            part = panel_ref[head, c].reshape(CHUNK, positions).astype(F32)
            at = pl.ds(pl.multiple_of(c * CHUNK, CHUNK), CHUNK)
            bias_ref[head, at, :] = part * (factor_ref[head] * LOG2E)

    def row_third(n):
        rows.arrive(n, 5, 6)
        rows.start(n, 9)

    def project(s):
        rows.arrive(s, 3, 4, 9)
        slot = lax.rem(s, 2)

        @pl.loop(0, chunks // 4)
        def _(group):
            for k in range(4):
                at = pl.ds(pl.multiple_of(group * (4 * CHUNK) + k * CHUNK, CHUNK), CHUNK)
                part = rows_ref[s, at, :]
                key = dot_nn(part, probe_ref[1]).astype(BF16)
                key_ref[2 * slot, at, :] = key[:, :HALF]
                key_ref[2 * slot + 1, at, :] = key[:, HALF:]
                value = dot_nt(switch_t_ref[...], part).astype(BF16)
                for head in range(HEADS):
                    value_ref[HEADS * slot + head, :WIDTH, at] = value[
                        head * WIDTH : (head + 1) * WIDTH
                    ]

        query = (dot_nt(probe_t_ref[...], rows_ref[s, own_spot, :]) * scale).astype(BF16)
        for head in range(HEADS):
            low = head % 4 * WIDTH
            query_ref[HEADS * slot + head, low : low + WIDTH, :] = query[
                head * WIDTH : (head + 1) * WIDTH
            ]

    QK, PV = 128, 256

    def scores(slot, head, into, c):
        at = pl.ds(c * QK, QK)
        part = dot_nn(key_ref[2 * slot + head // 4, at, :], query_ref[HEADS * slot + head])
        part = part + bias_ref[head, at, :]
        into[at, :] = part
        return jnp.max(part.reshape(QK // 8, 8, positions), axis=0)

    def highest(tops):
        return jnp.max(functools.reduce(jnp.maximum, tops), axis=0, keepdims=True)

    def step(slot, head, slot_next, head_next, source, into, top):
        total = jnp.zeros((VROWS, positions), F32)
        tops = []
        for c in range(keys // PV):
            for k in range(PV // QK):
                tops.append(scores(slot_next, head_next, into, c * (PV // QK) + k))
            at = pl.ds(c * PV, PV)
            weight = jnp.exp2(source[at, :] - top).astype(BF16)
            total = total + dot_nn(value_ref[HEADS * slot + head, :, at], weight)
        att_ref[slot, pl.ds(pl.multiple_of(head * WIDTH, WIDTH), WIDTH), :] = (
            total[:WIDTH] / total[WIDTH : WIDTH + 1]
        )
        return highest(tops)

    pairs = HEADS // 2
    steps = sequences * pairs

    bias.second(0)
    bias.second(1)
    rows.second(0)
    bias.second(2)
    rows.second(1)
    bias.second(3)
    rows.second(2)
    bias_third(0)
    rows.second(3)
    bias_third(1)
    rows.second(4)
    bias_third(2)
    bias_third(3)
    rows.second(5)
    bias_fourth(0)
    bias_fourth(1)
    row_third(0)
    bias_fourth(2)
    bias_fourth(3)
    project(0)
    bias_done(0)
    bias_done(1)
    max_ref[...] = highest([scores(0, 0, even_ref, c) for c in range(keys // QK)])

    @pl.loop(0, steps)
    def _(it):
        following = jnp.minimum(it + 1, steps - 1)
        s, pair = it // pairs, lax.rem(it, pairs)
        s_next, pair_next = following // pairs, lax.rem(following, pairs)
        slot, slot_next = lax.rem(s, 2), lax.rem(s_next, 2)

        def at_step(k, *actions):
            @pl.when(it == k)
            def _():
                for action, n in actions:
                    action(n)

        at_step(0, (rows.second, 6))
        at_step(1, (row_third, 1), (bias_done, 2))
        at_step(2, (rows.second, 7), (bias_done, 3))
        at_step(4, (row_third, 2))
        at_step(6, (row_third, 3))
        at_step(9, (row_third, 4))
        at_step(12, (row_third, 5))
        at_step(15, (row_third, 6))
        at_step(18, (row_third, 7))

        @pl.when((pair == 0) & (it > 0))
        def _():
            send_columns(s - 1)

        @pl.when(pair_next == 0)
        def _():
            project(s_next)

        head = pair * 2
        top = step(slot, head, slot, head + 1, even_ref, odd_ref, max_ref[...])
        max_ref[...] = step(slot, head + 1, slot_next, pair_next * 2, odd_ref, even_ref, top)

        @pl.when(pair == pairs - 1)
        def _():
            own = rows_ref[s, own_spot, :]
            gates = jax.nn.sigmoid(dot_nn(own, switch_ref[1]) + shift_ref[...])
            attended = (att_ref[slot].T * gates).astype(BF16)
            mixed = x_ref[s].astype(F32) + dot_nn(attended, final_ref[...])
            mixed_ref[s] = mixed
            stage_ref[s] = mixed.astype(BF16)
            columns_ref[seq * sequences + s] = stage_ref[
                s, pl.ds(pl.multiple_of(seq * residues, residues), residues), :
            ]

    send_columns(sequences - 1)

    @pl.loop(0, sequences)
    def _(n):
        rows.sent(n, *ROW_KINDS)

    @pl.loop(0, BIAS_PIECES)
    def _(n):
        bias.sent(n, *BIAS_KINDS)
        pair_copy(n, bias.core).wait_send()

    moved = columns_ref.at[pl.ds(0, sequences * (seq_count - 1))]
    every = pltpu.make_async_remote_copy(
        src_ref=moved,
        dst_ref=moved,
        send_sem=column_send,
        recv_sem=column_recv,
        device_id={"seq": twin},
        device_id_type=MESH,
    )
    every.wait_send()
    every.wait_recv()


def row_attention(x, prior, factor, norm, probe, switch, shift, final):
    sequences, positions, depth = x.shape
    keys = positions * lax.axis_size("res")
    seq_count = lax.axis_size("seq")
    vmem = pl.BlockSpec(memory_space=VM)
    dma = pltpu.SemaphoreType.DMA
    return pl.pallas_call(
        row_kernel,
        out_shape=[
            jax.ShapeDtypeStruct(x.shape, F32),
            jax.ShapeDtypeStruct((sequences * seq_count, positions // seq_count, depth), BF16),
        ],
        in_specs=[vmem, vmem, pl.BlockSpec(memory_space=pltpu.SMEM)] + [vmem] * 5,
        out_specs=[vmem, vmem],
        scratch_shapes=[
            VM((sequences, positions, depth), BF16),
            VM((sequences, keys, depth), BF16),
            VM((HEADS, seq_count // 2, 2, HALF, positions), BF16),
            VM((HEADS, keys, positions), F32),
            VM((keys, positions), F32),
            VM((keys, positions), F32),
            VM((4, keys, HALF), BF16),
            VM((2 * HEADS, VROWS, keys), BF16),
            VM((2 * HEADS, HALF, positions), BF16),
            VM((depth, depth), BF16),
            VM((depth, depth), BF16),
            VM((2, depth, positions), F32),
            VM((1, positions), F32),
            dma((sequences, 10)),
            dma((sequences, 10)),
            dma((BIAS_PIECES, 9)),
            dma((BIAS_PIECES, 9)),
            dma((BIAS_PIECES,)),
            dma((BIAS_PIECES,)),
            dma,
            dma,
        ],
        compiler_params=pltpu.CompilerParams(
            vmem_limit_bytes=66_000_000, collective_id=0, has_side_effects=True
        ),
    )(x, prior, factor, norm[None], probe, switch, shift[None], final)


def column_kernel(
    rows_ref, norm_ref, probe_ref, switch_ref, shift_ref, final_ref,
    back_ref,
    left_ref, right_ref, out_left_ref, out_right_ref, stage_ref, probe_t_ref, switch_t_ref,
    query_ref, att_ref,
    send_sem, recv_sem,
):
    count, residues, depth = rows_ref.shape
    seq = lax.axis_index("seq")
    seq_count = lax.axis_size("seq")
    sequences = back_ref.shape[0]
    part_size = stage_ref.shape[2]
    barrier = pltpu.get_barrier_semaphore()

    @pl.loop(1, seq_count)
    def _(k):
        peer = {"seq": lax.rem(seq + k, seq_count)}
        pl.semaphore_signal(barrier, inc=1, device_id=peer, device_id_type=MESH)

    probe_t_ref[...] = probe_ref[0].astype(F32).T.astype(BF16)
    switch_t_ref[...] = switch_ref[0].astype(F32).T.astype(BF16)
    query_ref[...] = jnp.zeros_like(query_ref)
    scale = LOG2E / math.sqrt(WIDTH)
    step = 16

    @pl.loop(0, count // step)
    def _(i):
        part = rows_ref[pl.ds(pl.multiple_of(i * step, step), step)].astype(F32)
        rows = step * residues
        part = standardize(part.reshape(rows, depth), norm_ref[...])
        at = pl.ds(pl.multiple_of(i * rows, rows), rows)
        left_ref[at, :] = part[:, :HALF]
        right_ref[at, :] = part[:, HALF:]

    ones = jnp.ones((16, count), BF16)

    def attend(r, slot):
        normed = jnp.concatenate(
            [
                jnp.concatenate(
                    [
                        left_ref[pl.ds(r + k, count, stride=residues), :],
                        right_ref[pl.ds(r + k, count, stride=residues), :],
                    ],
                    axis=1,
                )
                for k in range(2)
            ],
            axis=0,
        ).astype(BF16)
        key = dot_nn(normed, probe_ref[1]).astype(BF16)
        query = (dot_nt(probe_t_ref[...], normed) * scale).astype(BF16)
        value = dot_nt(switch_t_ref[...], normed).astype(BF16)
        gates = jax.nn.sigmoid(dot_nn(normed, switch_ref[1]) + shift_ref[...])
        for k in range(2):
            mine = slice(k * count, (k + 1) * count)
            for half in range(2):
                spot = 4 * slot + 2 * k + half
                for h in range(4):
                    low = h * WIDTH
                    query_ref[spot, low : low + WIDTH, h * count : (h + 1) * count] = query[
                        half * HALF + low : half * HALF + low + WIDTH, mine
                    ]
                score = dot_nn(key[mine, half * HALF : (half + 1) * HALF], query_ref[spot])
                top = jnp.max(score, axis=0, keepdims=True)
                weight = jnp.exp2(score - top).astype(BF16)
                for h in range(0, 4, 2):
                    low = half * HALF + h * WIDTH
                    block = jnp.concatenate([value[low : low + 2 * WIDTH, mine], ones], axis=0)
                    total = dot_nn(block, weight[:, h * count : (h + 2) * count])
                    for j in range(2):
                        spread = slice(j * count, (j + 1) * count)
                        att_ref[
                            slot, low + j * WIDTH : low + (j + 1) * WIDTH, k * count : (k + 1) * count
                        ] = (
                            total[j * WIDTH : (j + 1) * WIDTH, spread]
                            / total[2 * WIDTH : 2 * WIDTH + 1, spread]
                        )
        attended = (att_ref[slot].T * gates).astype(BF16)
        return dot_nn(attended, final_ref[...])

    def back_copy(part, target):
        return pltpu.make_async_remote_copy(
            src_ref=stage_ref.at[part, pl.ds(target * sequences, sequences)],
            dst_ref=back_ref.at[
                :, pl.ds(pl.multiple_of(seq * residues + part * part_size, part_size), part_size), :
            ],
            send_sem=send_sem,
            recv_sem=recv_sem,
            device_id={"seq": target},
            device_id_type=MESH,
        )

    pairs = 2
    for part in range(residues // part_size):

        @pl.loop(0, part_size // (2 * pairs))
        def _(group):
            low = group * (2 * pairs)
            deltas = [attend(part * part_size + low + 2 * p, p) for p in range(pairs)]
            for p, delta in enumerate(deltas):
                for k in range(2):
                    spots = pl.ds(low + 2 * p + k, count, stride=part_size)
                    out_left_ref[spots, :] = delta[k * count : (k + 1) * count, :HALF]
                    out_right_ref[spots, :] = delta[k * count : (k + 1) * count, HALF:]

        @pl.loop(0, count // step)
        def _(i):
            rows = step * part_size
            at = pl.ds(pl.multiple_of(i * rows, rows), rows)
            block = jnp.concatenate([out_left_ref[at, :], out_right_ref[at, :]], axis=1)
            stage_ref[part, pl.ds(pl.multiple_of(i * step, step), step)] = block.astype(BF16).reshape(
                step, part_size, depth
            )

        if part == 0:
            pl.semaphore_wait(barrier, seq_count - 1)

        @pl.loop(1, seq_count)
        def _(k):
            back_copy(part, lax.rem(seq + k, seq_count)).start()

        back_ref[
            :, pl.ds(pl.multiple_of(seq * residues + part * part_size, part_size), part_size), :
        ] = stage_ref[part, pl.ds(seq * sequences, sequences)]

    moved = back_ref.at[:, pl.ds(0, residues * (seq_count - 1)), :]
    every = pltpu.make_async_remote_copy(
        src_ref=moved,
        dst_ref=moved,
        send_sem=send_sem,
        recv_sem=recv_sem,
        device_id={"seq": lax.rem(seq + 1, seq_count)},
        device_id_type=MESH,
    )
    every.wait_send()
    every.wait_recv()


def column_attention(rows, norm, probe, switch, shift, final):
    count, residues, depth = rows.shape
    seq_count = lax.axis_size("seq")
    part_size = residues // 2
    vmem = pl.BlockSpec(memory_space=VM)
    dma = pltpu.SemaphoreType.DMA
    return pl.pallas_call(
        column_kernel,
        out_shape=jax.ShapeDtypeStruct((count // seq_count, residues * seq_count, depth), BF16),
        in_specs=[vmem] * 6,
        out_specs=vmem,
        scratch_shapes=[
            VM((count * residues, HALF), F32),
            VM((count * residues, HALF), F32),
            VM((count * part_size, HALF), F32),
            VM((count * part_size, HALF), F32),
            VM((residues // part_size, count, part_size, depth), BF16),
            VM((depth, depth), BF16),
            VM((depth, depth), BF16),
            VM((8, HALF, 4 * count), BF16),
            VM((2, depth, 2 * count), F32),
            dma,
            dma,
        ],
        compiler_params=pltpu.CompilerParams(collective_id=1, has_side_effects=True),
    )(rows, norm[None], probe, switch, shift[None], final)


def shards(x, prior, factor, norm_h, probe_h, switch_h, shift_h, final_h, norm_v, probe_v, switch_v, shift_v, final_v):
    mixed, columns = row_attention(x, prior, factor, norm_h, probe_h, switch_h, shift_h, final_h)
    back = column_attention(columns, norm_v, probe_v, switch_v, shift_v, final_v)
    return mixed + back.astype(F32)


def solution(mesh):
    placed = (P("seq", "res", None), P(None, "res", "seq")) + (P(),) * 11
    return jax.shard_map(
        shards, mesh=mesh, in_specs=placed, out_specs=P("seq", "res", None), check_vma=False
    )
```

```python
import functools
import math

import jax
import jax.numpy as jnp
from jax import lax
from jax.experimental import pallas as pl
from jax.experimental.pallas import tpu as pltpu
from jax.sharding import PartitionSpec as P

EPS = 1e-05
LOG2E = 1.4426950408889634
F32 = jnp.float32
BF16 = jnp.bfloat16
HEADS = 8
WIDTH = 32
HALF = 128
VROWS = 48
CHUNK = 256
VM = pltpu.VMEM


def dot_nn(a, b):
    return lax.dot_general(a, b, (((1,), (0,)), ((), ())), preferred_element_type=F32)


def dot_nt(a, b):
    return lax.dot_general(a, b, (((1,), (1,)), ((), ())), preferred_element_type=F32)


def standardize(x, factor):
    mean = jnp.sum(x, -1, keepdims=True) * (1.0 / x.shape[-1])
    centred = x - mean
    var = jnp.sum(centred * centred, -1, keepdims=True) * (1.0 / x.shape[-1])
    return centred * lax.rsqrt(var + EPS) * factor


MESH = pl.DeviceIdType.MESH
RING = 4


class Exchange:
    def __init__(self, axis, cores, view, send, recv):
        index = lax.axis_index(axis)
        self.axis, self.cores, self.view, self.send, self.recv = axis, cores, view, send, recv
        self.core = lax.rem(index, cores)
        chip = index // cores
        self.ring, self.at = chip // RING, lax.rem(chip, RING)
        self.mirror = self.device(1 - self.ring, 0)
        self.up, self.down = self.device(self.ring, 1), self.device(self.ring, -1)

    def block(self, ring, shift):
        return ring * RING + lax.rem(self.at + (shift + RING), RING)

    def device(self, ring, shift):
        return self.block(ring, shift) * self.cores + self.core

    def peers(self):
        return [{self.axis: d} for d in (self.mirror, self.up, self.down)]

    def plan(self, kind):
        mine, other = self.ring, 1 - self.ring
        return {
            0: ((mine, 0, None), self.mirror, (other, 0, None)),
            1: ((mine, 0, None), self.up, (mine, -1, None)),
            2: ((mine, 0, None), self.down, (mine, 1, None)),
            3: ((other, 0, None), self.up, (other, -1, None)),
            4: ((other, 0, None), self.down, (other, 1, None)),
            5: ((mine, -1, 0), self.up, (mine, -2, 0)),
            6: ((mine, 1, 1), self.down, (mine, 2, 1)),
            7: ((other, -1, 0), self.up, (other, -2, 0)),
            8: ((other, 1, 1), self.down, (other, 2, 1)),
            9: ((mine, 2, None), self.mirror, (other, 2, None)),
        }[kind]

    def copy(self, n, kind, incoming):
        out, target, into = self.plan(kind)
        ring, shift, half = into if incoming else out
        view = self.view(n, self.block(ring, shift), half)
        return pltpu.make_async_remote_copy(
            src_ref=view,
            dst_ref=view,
            send_sem=self.send.at[n, kind],
            recv_sem=self.recv.at[n, kind],
            device_id={self.axis: target},
            device_id_type=MESH,
        )

    def start(self, n, *kinds):
        for kind in kinds:
            self.copy(n, kind, False).start()

    def arrive(self, n, *kinds):
        for kind in kinds:
            self.copy(n, kind, True).wait_recv()

    def sent(self, n, *kinds):
        for kind in kinds:
            self.copy(n, kind, False).wait_send()

    def first(self, n):
        self.start(n, 0, 1, 2)

    def second(self, n):
        self.arrive(n, 0)
        self.start(n, 3, 4)
        self.arrive(n, 1)
        self.start(n, 5)
        self.arrive(n, 2)
        self.start(n, 6)


BIAS_PIECES = 4
BIAS_KINDS = (0, 1, 2, 3, 4, 5, 6, 7, 8)
ROW_KINDS = (0, 1, 2, 3, 4, 5, 6, 9)


def row_kernel(
    x_ref, prior_ref, factor_ref, norm_ref, probe_ref, switch_ref, shift_ref, final_ref,
    norm_v_ref, probe_v_ref, switch_v_ref, shift_v_ref, final_v_ref,
    mixed_ref, back_ref,
    columns_ref, stage_ref, rows_ref, panel_ref, bias_ref, even_ref, odd_ref, key_ref, value_ref, query_ref, probe_t_ref,
    switch_t_ref, att_ref, max_ref,
    left_ref, right_ref, out_left_ref, out_right_ref, delta_ref, column_query_ref, column_att_ref,
    row_send, row_recv, bias_send, bias_recv, pair_send, pair_recv, column_send, column_recv,
    back_send, back_recv,
):
    sequences, positions, depth = x_ref.shape
    keys = rows_ref.shape[1]
    chunks = keys // CHUNK
    res = lax.axis_index("res")
    per_piece = HEADS // BIAS_PIECES

    def row_view(n, block, half):
        size = positions if half is None else positions // 2
        low = block * positions + (0 if half is None else half * size)
        return rows_ref.at[n, pl.ds(pl.multiple_of(low, HALF), size), :]

    def bias_view(n, block, half):
        size = HALF if half is None else HALF // 2
        low = 0 if half is None else half * size
        return panel_ref.at[pl.ds(n * per_piece, per_piece), block, bias.core, pl.ds(low, size), :]

    rows = Exchange("res", 1, row_view, row_send, row_recv)
    bias = Exchange("seq", 2, bias_view, bias_send, bias_recv)
    twin = lax.axis_index("seq") + 1 - 2 * bias.core

    def pair_copy(n, core):
        view = panel_ref.at[pl.ds(n * per_piece, per_piece), :, core]
        return pltpu.make_async_remote_copy(
            src_ref=view,
            dst_ref=view,
            send_sem=pair_send.at[n],
            recv_sem=pair_recv.at[n],
            device_id={"seq": twin},
            device_id_type=MESH,
        )

    seq = lax.axis_index("seq")
    seq_count = columns_ref.shape[0] // sequences
    residues = columns_ref.shape[1]

    def column_copy(n, target):
        return pltpu.make_async_remote_copy(
            src_ref=stage_ref.at[n, pl.ds(pl.multiple_of(target * residues, residues), residues), :],
            dst_ref=columns_ref.at[seq * sequences + n],
            send_sem=column_send,
            recv_sem=column_recv,
            device_id={"seq": target},
            device_id_type=MESH,
        )

    def send_columns(n):
        @pl.loop(1, seq_count)
        def _(k):
            column_copy(n, lax.rem(seq + k, seq_count)).start()

    barrier = pltpu.get_barrier_semaphore()
    for peer in rows.peers():
        pl.semaphore_signal(barrier, inc=1, device_id=peer, device_id_type=MESH)

    @pl.loop(1, seq_count)
    def _(k):
        peer = {"seq": lax.rem(seq + k, seq_count)}
        pl.semaphore_signal(barrier, inc=1, device_id=peer, device_id_type=MESH)

    for head in range(HEADS):
        panel_ref[head, bias.block(bias.ring, 0), bias.core] = (
            prior_ref[head].astype(F32).T.astype(BF16)
        )

    own_spot = pl.ds(pl.multiple_of(res * positions, positions), positions)

    @pl.loop(0, sequences)
    def _(s):
        rows_ref[s, own_spot, :] = standardize(x_ref[s].astype(F32), norm_ref[...]).astype(BF16)

    pl.semaphore_wait(barrier, 3 + seq_count - 1)
    for n in range(BIAS_PIECES):
        bias.first(n)
    for n in range(sequences):
        rows.first(n)

    probe_t_ref[...] = probe_ref[0].astype(F32).T.astype(BF16)
    switch_t_ref[...] = switch_ref[0].astype(F32).T.astype(BF16)
    query_ref[...] = jnp.zeros_like(query_ref)
    scale = LOG2E / math.sqrt(WIDTH)

    @pl.loop(0, 2 * HEADS)
    def _(spot):
        value_ref[spot, WIDTH:, :] = jnp.ones((VROWS - WIDTH, keys), BF16)

    def bias_third(n):
        bias.arrive(n, 3)
        bias.start(n, 7)
        bias.arrive(n, 4)
        bias.start(n, 8)

    def bias_fourth(n):
        bias.arrive(n, 5, 6, 7, 8)
        pair_copy(n, bias.core).start()

    def bias_done(n):
        pair_copy(n, 1 - bias.core).wait_recv()

        @pl.loop(0, per_piece * chunks)
        def _(k):
            head = n * per_piece + k // chunks
            c = lax.rem(k, chunks)
            part = panel_ref[head, c].reshape(CHUNK, positions).astype(F32)
            at = pl.ds(pl.multiple_of(c * CHUNK, CHUNK), CHUNK)
            bias_ref[head, at, :] = part * (factor_ref[head] * LOG2E)

    def row_third(n):
        rows.arrive(n, 5, 6)
        rows.start(n, 9)

    def project(s):
        rows.arrive(s, 3, 4, 9)
        slot = lax.rem(s, 2)

        @pl.loop(0, chunks // 4)
        def _(group):
            for k in range(4):
                at = pl.ds(pl.multiple_of(group * (4 * CHUNK) + k * CHUNK, CHUNK), CHUNK)
                part = rows_ref[s, at, :]
                key = dot_nn(part, probe_ref[1]).astype(BF16)
                key_ref[2 * slot, at, :] = key[:, :HALF]
                key_ref[2 * slot + 1, at, :] = key[:, HALF:]
                value = dot_nt(switch_t_ref[...], part).astype(BF16)
                for head in range(HEADS):
                    value_ref[HEADS * slot + head, :WIDTH, at] = value[
                        head * WIDTH : (head + 1) * WIDTH
                    ]

        query = (dot_nt(probe_t_ref[...], rows_ref[s, own_spot, :]) * scale).astype(BF16)
        for head in range(HEADS):
            low = head % 4 * WIDTH
            query_ref[HEADS * slot + head, low : low + WIDTH, :] = query[
                head * WIDTH : (head + 1) * WIDTH
            ]

    QK, PV = 128, 256

    def scores(slot, head, into, c):
        at = pl.ds(c * QK, QK)
        part = dot_nn(key_ref[2 * slot + head // 4, at, :], query_ref[HEADS * slot + head])
        part = part + bias_ref[head, at, :]
        into[at, :] = part
        return jnp.max(part.reshape(QK // 8, 8, positions), axis=0)

    def highest(tops):
        return jnp.max(functools.reduce(jnp.maximum, tops), axis=0, keepdims=True)

    def step(slot, head, slot_next, head_next, source, into, top):
        total = jnp.zeros((VROWS, positions), F32)
        tops = []
        for c in range(keys // PV):
            for k in range(PV // QK):
                tops.append(scores(slot_next, head_next, into, c * (PV // QK) + k))
            at = pl.ds(c * PV, PV)
            weight = jnp.exp2(source[at, :] - top).astype(BF16)
            total = total + dot_nn(value_ref[HEADS * slot + head, :, at], weight)
        att_ref[slot, pl.ds(pl.multiple_of(head * WIDTH, WIDTH), WIDTH), :] = (
            total[:WIDTH] / total[WIDTH : WIDTH + 1]
        )
        return highest(tops)

    pairs = HEADS // 2
    steps = sequences * pairs

    bias.second(0)
    bias.second(1)
    rows.second(0)
    bias.second(2)
    rows.second(1)
    bias.second(3)
    rows.second(2)
    bias_third(0)
    rows.second(3)
    bias_third(1)
    rows.second(4)
    bias_third(2)
    bias_third(3)
    rows.second(5)
    bias_fourth(0)
    bias_fourth(1)
    row_third(0)
    bias_fourth(2)
    bias_fourth(3)
    project(0)
    bias_done(0)
    bias_done(1)
    max_ref[...] = highest([scores(0, 0, even_ref, c) for c in range(keys // QK)])

    @pl.loop(0, steps)
    def _(it):
        following = jnp.minimum(it + 1, steps - 1)
        s, pair = it // pairs, lax.rem(it, pairs)
        s_next, pair_next = following // pairs, lax.rem(following, pairs)
        slot, slot_next = lax.rem(s, 2), lax.rem(s_next, 2)

        def at_step(k, *actions):
            @pl.when(it == k)
            def _():
                for action, n in actions:
                    action(n)

        at_step(0, (rows.second, 6))
        at_step(1, (row_third, 1), (bias_done, 2))
        at_step(2, (rows.second, 7), (bias_done, 3))
        at_step(4, (row_third, 2))
        at_step(6, (row_third, 3))
        at_step(9, (row_third, 4))
        at_step(12, (row_third, 5))
        at_step(15, (row_third, 6))
        at_step(18, (row_third, 7))

        @pl.when((pair == 0) & (it > 0))
        def _():
            send_columns(s - 1)

        @pl.when(pair_next == 0)
        def _():
            project(s_next)

        head = pair * 2
        top = step(slot, head, slot, head + 1, even_ref, odd_ref, max_ref[...])
        max_ref[...] = step(slot, head + 1, slot_next, pair_next * 2, odd_ref, even_ref, top)

        @pl.when(pair == pairs - 1)
        def _():
            own = rows_ref[s, own_spot, :]
            gates = jax.nn.sigmoid(dot_nn(own, switch_ref[1]) + shift_ref[...])
            attended = (att_ref[slot].T * gates).astype(BF16)
            mixed = x_ref[s].astype(F32) + dot_nn(attended, final_ref[...])
            mixed_ref[s] = mixed
            stage_ref[s] = mixed.astype(BF16)
            columns_ref[seq * sequences + s] = stage_ref[
                s, pl.ds(pl.multiple_of(seq * residues, residues), residues), :
            ]

    send_columns(sequences - 1)

    moved = columns_ref.at[pl.ds(0, sequences * (seq_count - 1))]
    every = pltpu.make_async_remote_copy(
        src_ref=moved,
        dst_ref=moved,
        send_sem=column_send,
        recv_sem=column_recv,
        device_id={"seq": twin},
        device_id_type=MESH,
    )
    every.wait_recv()
    column_phase(
        columns_ref, norm_v_ref, probe_v_ref, switch_v_ref, shift_v_ref, final_v_ref,
        back_ref,
        left_ref, right_ref, out_left_ref, out_right_ref, delta_ref, probe_t_ref, switch_t_ref,
        column_query_ref, column_att_ref,
        back_send, back_recv,
    )
    every.wait_send()

    @pl.loop(0, sequences)
    def _(n):
        rows.sent(n, *ROW_KINDS)

    @pl.loop(0, BIAS_PIECES)
    def _(n):
        bias.sent(n, *BIAS_KINDS)
        pair_copy(n, bias.core).wait_send()


def attention(
    x, prior, factor, norm, probe, switch, shift, final, norm_v, probe_v, switch_v, shift_v, final_v
):
    sequences, positions, depth = x.shape
    keys = positions * lax.axis_size("res")
    seq_count = lax.axis_size("seq")
    count, residues = sequences * seq_count, positions // seq_count
    part_size = residues // 2
    vmem = pl.BlockSpec(memory_space=VM)
    dma = pltpu.SemaphoreType.DMA
    return pl.pallas_call(
        row_kernel,
        out_shape=[
            jax.ShapeDtypeStruct(x.shape, F32),
            jax.ShapeDtypeStruct(x.shape, BF16),
        ],
        in_specs=[vmem, vmem, pl.BlockSpec(memory_space=pltpu.SMEM)] + [vmem] * 10,
        out_specs=[vmem, vmem],
        scratch_shapes=[
            VM((count, residues, depth), BF16),
            VM((sequences, positions, depth), BF16),
            VM((sequences, keys, depth), BF16),
            VM((HEADS, seq_count // 2, 2, HALF, positions), BF16),
            VM((HEADS, keys, positions), F32),
            VM((keys, positions), F32),
            VM((keys, positions), F32),
            VM((4, keys, HALF), BF16),
            VM((2 * HEADS, VROWS, keys), BF16),
            VM((2 * HEADS, HALF, positions), BF16),
            VM((depth, depth), BF16),
            VM((depth, depth), BF16),
            VM((2, depth, positions), F32),
            VM((1, positions), F32),
            VM((count * residues, HALF), F32),
            VM((count * residues, HALF), F32),
            VM((count * part_size, HALF), F32),
            VM((count * part_size, HALF), F32),
            VM((residues // part_size, count, part_size, depth), BF16),
            VM((8, HALF, 4 * count), BF16),
            VM((2, depth, 2 * count), F32),
            dma((sequences, 10)),
            dma((sequences, 10)),
            dma((BIAS_PIECES, 9)),
            dma((BIAS_PIECES, 9)),
            dma((BIAS_PIECES,)),
            dma((BIAS_PIECES,)),
            dma,
            dma,
            dma,
            dma,
        ],
        compiler_params=pltpu.CompilerParams(
            vmem_limit_bytes=66_000_000, collective_id=0, has_side_effects=True
        ),
    )(
        x, prior, factor, norm[None], probe, switch, shift[None], final,
        norm_v[None], probe_v, switch_v, shift_v[None], final_v,
    )


def column_phase(
    rows_ref, norm_ref, probe_ref, switch_ref, shift_ref, final_ref,
    back_ref,
    left_ref, right_ref, out_left_ref, out_right_ref, stage_ref, probe_t_ref, switch_t_ref,
    query_ref, att_ref,
    send_sem, recv_sem,
):
    count, residues, depth = rows_ref.shape
    seq = lax.axis_index("seq")
    seq_count = lax.axis_size("seq")
    sequences = back_ref.shape[0]
    part_size = stage_ref.shape[2]
    probe_t_ref[...] = probe_ref[0].astype(F32).T.astype(BF16)
    switch_t_ref[...] = switch_ref[0].astype(F32).T.astype(BF16)
    query_ref[...] = jnp.zeros_like(query_ref)
    scale = LOG2E / math.sqrt(WIDTH)
    step = 16

    @pl.loop(0, count // step)
    def _(i):
        part = rows_ref[pl.ds(pl.multiple_of(i * step, step), step)].astype(F32)
        rows = step * residues
        part = standardize(part.reshape(rows, depth), norm_ref[...])
        at = pl.ds(pl.multiple_of(i * rows, rows), rows)
        left_ref[at, :] = part[:, :HALF]
        right_ref[at, :] = part[:, HALF:]

    ones = jnp.ones((16, count), BF16)

    def attend(r, slot):
        normed = jnp.concatenate(
            [
                jnp.concatenate(
                    [
                        left_ref[pl.ds(r + k, count, stride=residues), :],
                        right_ref[pl.ds(r + k, count, stride=residues), :],
                    ],
                    axis=1,
                )
                for k in range(2)
            ],
            axis=0,
        ).astype(BF16)
        key = dot_nn(normed, probe_ref[1]).astype(BF16)
        query = (dot_nt(probe_t_ref[...], normed) * scale).astype(BF16)
        value = dot_nt(switch_t_ref[...], normed).astype(BF16)
        gates = jax.nn.sigmoid(dot_nn(normed, switch_ref[1]) + shift_ref[...])
        for k in range(2):
            mine = slice(k * count, (k + 1) * count)
            for half in range(2):
                spot = 4 * slot + 2 * k + half
                for h in range(4):
                    low = h * WIDTH
                    query_ref[spot, low : low + WIDTH, h * count : (h + 1) * count] = query[
                        half * HALF + low : half * HALF + low + WIDTH, mine
                    ]
                score = dot_nn(key[mine, half * HALF : (half + 1) * HALF], query_ref[spot])
                top = jnp.max(score, axis=0, keepdims=True)
                weight = jnp.exp2(score - top).astype(BF16)
                for h in range(0, 4, 2):
                    low = half * HALF + h * WIDTH
                    block = jnp.concatenate([value[low : low + 2 * WIDTH, mine], ones], axis=0)
                    total = dot_nn(block, weight[:, h * count : (h + 2) * count])
                    for j in range(2):
                        spread = slice(j * count, (j + 1) * count)
                        att_ref[
                            slot, low + j * WIDTH : low + (j + 1) * WIDTH, k * count : (k + 1) * count
                        ] = (
                            total[j * WIDTH : (j + 1) * WIDTH, spread]
                            / total[2 * WIDTH : 2 * WIDTH + 1, spread]
                        )
        attended = (att_ref[slot].T * gates).astype(BF16)
        return dot_nn(attended, final_ref[...])

    def back_copy(part, target):
        return pltpu.make_async_remote_copy(
            src_ref=stage_ref.at[part, pl.ds(target * sequences, sequences)],
            dst_ref=back_ref.at[
                :, pl.ds(pl.multiple_of(seq * residues + part * part_size, part_size), part_size), :
            ],
            send_sem=send_sem,
            recv_sem=recv_sem,
            device_id={"seq": target},
            device_id_type=MESH,
        )

    pairs = 2
    for part in range(residues // part_size):

        @pl.loop(0, part_size // (2 * pairs))
        def _(group):
            low = group * (2 * pairs)
            deltas = [attend(part * part_size + low + 2 * p, p) for p in range(pairs)]
            for p, delta in enumerate(deltas):
                for k in range(2):
                    spots = pl.ds(low + 2 * p + k, count, stride=part_size)
                    out_left_ref[spots, :] = delta[k * count : (k + 1) * count, :HALF]
                    out_right_ref[spots, :] = delta[k * count : (k + 1) * count, HALF:]

        @pl.loop(0, count // step)
        def _(i):
            rows = step * part_size
            at = pl.ds(pl.multiple_of(i * rows, rows), rows)
            block = jnp.concatenate([out_left_ref[at, :], out_right_ref[at, :]], axis=1)
            stage_ref[part, pl.ds(pl.multiple_of(i * step, step), step)] = block.astype(BF16).reshape(
                step, part_size, depth
            )

        @pl.loop(1, seq_count)
        def _(k):
            back_copy(part, lax.rem(seq + k, seq_count)).start()

        back_ref[
            :, pl.ds(pl.multiple_of(seq * residues + part * part_size, part_size), part_size), :
        ] = stage_ref[part, pl.ds(seq * sequences, sequences)]

    moved = back_ref.at[:, pl.ds(0, residues * (seq_count - 1)), :]
    every = pltpu.make_async_remote_copy(
        src_ref=moved,
        dst_ref=moved,
        send_sem=send_sem,
        recv_sem=recv_sem,
        device_id={"seq": lax.rem(seq + 1, seq_count)},
        device_id_type=MESH,
    )
    every.wait_send()
    every.wait_recv()


def shards(x, prior, factor, norm_h, probe_h, switch_h, shift_h, final_h, norm_v, probe_v, switch_v, shift_v, final_v):
    mixed, back = attention(
        x, prior, factor, norm_h, probe_h, switch_h, shift_h, final_h, norm_v, probe_v, switch_v, shift_v, final_v
    )
    return mixed + back.astype(F32)


def solution(mesh):
    placed = (P("seq", "res", None), P(None, "res", "seq")) + (P(),) * 11
    return jax.shard_map(
        shards, mesh=mesh, in_specs=placed, out_specs=P("seq", "res", None), check_vma=False
    )
```

```python
import functools
import math

import jax
import jax.numpy as jnp
from jax import lax
from jax.experimental import pallas as pl
from jax.experimental.pallas import tpu as pltpu
from jax.sharding import PartitionSpec as P

EPS = 1e-05
LOG2E = 1.4426950408889634
F32 = jnp.float32
BF16 = jnp.bfloat16
HEADS = 8
WIDTH = 32
HALF = 128
VROWS = 48
CHUNK = 256
VM = pltpu.VMEM


def dot_nn(a, b):
    return lax.dot_general(a, b, (((1,), (0,)), ((), ())), preferred_element_type=F32)


def dot_nt(a, b):
    return lax.dot_general(a, b, (((1,), (1,)), ((), ())), preferred_element_type=F32)


def standardize(x, factor):
    mean = jnp.sum(x, -1, keepdims=True) * (1.0 / x.shape[-1])
    centred = x - mean
    var = jnp.sum(centred * centred, -1, keepdims=True) * (1.0 / x.shape[-1])
    return centred * lax.rsqrt(var + EPS) * factor


MESH = pl.DeviceIdType.MESH
RING = 4


class Exchange:
    def __init__(self, axis, cores, view, send, recv):
        index = lax.axis_index(axis)
        self.axis, self.cores, self.view, self.send, self.recv = axis, cores, view, send, recv
        self.core = lax.rem(index, cores)
        chip = index // cores
        self.ring, self.at = chip // RING, lax.rem(chip, RING)
        self.mirror = self.device(1 - self.ring, 0)
        self.up, self.down = self.device(self.ring, 1), self.device(self.ring, -1)

    def block(self, ring, shift):
        return ring * RING + lax.rem(self.at + (shift + RING), RING)

    def device(self, ring, shift):
        return self.block(ring, shift) * self.cores + self.core

    def peers(self):
        return [{self.axis: d} for d in (self.mirror, self.up, self.down)]

    def plan(self, kind):
        mine, other = self.ring, 1 - self.ring
        return {
            0: ((mine, 0, None), self.mirror, (other, 0, None)),
            1: ((mine, 0, None), self.up, (mine, -1, None)),
            2: ((mine, 0, None), self.down, (mine, 1, None)),
            3: ((other, 0, None), self.up, (other, -1, None)),
            4: ((other, 0, None), self.down, (other, 1, None)),
            5: ((mine, -1, 0), self.up, (mine, -2, 0)),
            6: ((mine, 1, 1), self.down, (mine, 2, 1)),
            7: ((other, -1, 0), self.up, (other, -2, 0)),
            8: ((other, 1, 1), self.down, (other, 2, 1)),
            9: ((mine, 2, None), self.mirror, (other, 2, None)),
        }[kind]

    def copy(self, n, kind, incoming):
        out, target, into = self.plan(kind)
        ring, shift, half = into if incoming else out
        view = self.view(n, self.block(ring, shift), half)
        return pltpu.make_async_remote_copy(
            src_ref=view,
            dst_ref=view,
            send_sem=self.send.at[n, kind],
            recv_sem=self.recv.at[n, kind],
            device_id={self.axis: target},
            device_id_type=MESH,
        )

    def start(self, n, *kinds):
        for kind in kinds:
            self.copy(n, kind, False).start()

    def arrive(self, n, *kinds):
        for kind in kinds:
            self.copy(n, kind, True).wait_recv()

    def sent(self, n, *kinds):
        for kind in kinds:
            self.copy(n, kind, False).wait_send()

    def first(self, n):
        self.start(n, 0, 1, 2)

    def second(self, n):
        self.arrive(n, 0)
        self.start(n, 3, 4)
        self.arrive(n, 1)
        self.start(n, 5)
        self.arrive(n, 2)
        self.start(n, 6)


BIAS_PIECES = 4
BIAS_KINDS = (0, 1, 2, 3, 4, 5, 6, 7, 8)
ROW_KINDS = (0, 1, 2, 3, 4, 5, 6, 9)


def row_kernel(
    x_ref, prior_ref, factor_ref, norm_ref, probe_ref, switch_ref, shift_ref, final_ref,
    norm_v_ref, probe_v_ref, switch_v_ref, shift_v_ref, final_v_ref,
    mixed_ref, back_ref,
    columns_ref, stage_ref, rows_ref, panel_ref, bias_ref, even_ref, odd_ref, key_ref, value_ref, query_ref, probe_t_ref,
    switch_t_ref, att_ref, max_ref,
    left_ref, right_ref, out_left_ref, out_right_ref, delta_ref, column_query_ref, column_att_ref,
    row_send, row_recv, bias_send, bias_recv, pair_send, pair_recv, column_send, column_recv,
    back_send, back_recv,
):
    sequences, positions, depth = x_ref.shape
    keys = rows_ref.shape[1]
    chunks = keys // CHUNK
    res = lax.axis_index("res")
    per_piece = HEADS // BIAS_PIECES

    def row_view(n, block, half):
        size = positions if half is None else positions // 2
        low = block * positions + (0 if half is None else half * size)
        return rows_ref.at[n, pl.ds(pl.multiple_of(low, HALF), size), :]

    def bias_view(n, block, half):
        size = HALF if half is None else HALF // 2
        low = 0 if half is None else half * size
        return panel_ref.at[pl.ds(n * per_piece, per_piece), block, bias.core, pl.ds(low, size), :]

    rows = Exchange("res", 1, row_view, row_send, row_recv)
    bias = Exchange("seq", 2, bias_view, bias_send, bias_recv)
    twin = lax.axis_index("seq") + 1 - 2 * bias.core

    def pair_copy(n, core):
        view = panel_ref.at[pl.ds(n * per_piece, per_piece), :, core]
        return pltpu.make_async_remote_copy(
            src_ref=view,
            dst_ref=view,
            send_sem=pair_send.at[n],
            recv_sem=pair_recv.at[n],
            device_id={"seq": twin},
            device_id_type=MESH,
        )

    seq = lax.axis_index("seq")
    seq_count = columns_ref.shape[0] // sequences
    residues = columns_ref.shape[1]

    def column_copy(n, target):
        return pltpu.make_async_remote_copy(
            src_ref=stage_ref.at[n, pl.ds(pl.multiple_of(target * residues, residues), residues), :],
            dst_ref=columns_ref.at[seq * sequences + n],
            send_sem=column_send,
            recv_sem=column_recv,
            device_id={"seq": target},
            device_id_type=MESH,
        )

    def send_columns(n):
        @pl.loop(1, seq_count)
        def _(k):
            column_copy(n, lax.rem(seq + k, seq_count)).start()

    barrier = pltpu.get_barrier_semaphore()
    for peer in rows.peers():
        pl.semaphore_signal(barrier, inc=1, device_id=peer, device_id_type=MESH)

    @pl.loop(1, seq_count)
    def _(k):
        peer = {"seq": lax.rem(seq + k, seq_count)}
        pl.semaphore_signal(barrier, inc=1, device_id=peer, device_id_type=MESH)

    for head in range(HEADS):
        panel_ref[head, bias.block(bias.ring, 0), bias.core] = (
            prior_ref[head].astype(F32).T.astype(BF16)
        )

    own_spot = pl.ds(pl.multiple_of(res * positions, positions), positions)

    @pl.loop(0, sequences)
    def _(s):
        rows_ref[s, own_spot, :] = standardize(x_ref[s].astype(F32), norm_ref[...]).astype(BF16)

    pl.semaphore_wait(barrier, 3 + seq_count - 1)
    for n in range(BIAS_PIECES):
        bias.first(n)
    for n in range(sequences):
        rows.first(n)

    probe_t_ref[...] = probe_ref[0].astype(F32).T.astype(BF16)
    switch_t_ref[...] = switch_ref[0].astype(F32).T.astype(BF16)
    query_ref[...] = jnp.zeros_like(query_ref)
    scale = LOG2E / math.sqrt(WIDTH)

    @pl.loop(0, 2 * HEADS)
    def _(spot):
        value_ref[spot, WIDTH:, :] = jnp.ones((VROWS - WIDTH, keys), BF16)

    def bias_third(n):
        bias.arrive(n, 3)
        bias.start(n, 7)
        bias.arrive(n, 4)
        bias.start(n, 8)

    def bias_fourth(n):
        bias.arrive(n, 5, 6, 7, 8)
        pair_copy(n, bias.core).start()

    def bias_done(n):
        pair_copy(n, 1 - bias.core).wait_recv()

        @pl.loop(0, per_piece * chunks)
        def _(k):
            head = n * per_piece + k // chunks
            c = lax.rem(k, chunks)
            part = panel_ref[head, c].reshape(CHUNK, positions).astype(F32)
            at = pl.ds(pl.multiple_of(c * CHUNK, CHUNK), CHUNK)
            bias_ref[head, at, :] = part * (factor_ref[head] * LOG2E)

    def row_third(n):
        rows.arrive(n, 5, 6)
        rows.start(n, 9)

    def project(s):
        rows.arrive(s, 3, 4, 9)
        slot = lax.rem(s, 2)

        for c in range(chunks):
            at = pl.ds(c * CHUNK, CHUNK)
            part = rows_ref[s, at, :]
            key = dot_nn(part, probe_ref[1]).astype(BF16)
            key_ref[2 * slot, at, :] = key[:, :HALF]
            key_ref[2 * slot + 1, at, :] = key[:, HALF:]
            value = dot_nt(switch_t_ref[...], part).astype(BF16)
            for head in range(HEADS):
                value_ref[HEADS * slot + head, :WIDTH, at] = value[head * WIDTH : (head + 1) * WIDTH]

        query = (dot_nt(probe_t_ref[...], rows_ref[s, own_spot, :]) * scale).astype(BF16)
        for head in range(HEADS):
            low = head % 4 * WIDTH
            query_ref[HEADS * slot + head, low : low + WIDTH, :] = query[
                head * WIDTH : (head + 1) * WIDTH
            ]

    QK, PV = 128, 256

    def scores(slot, head, into, c):
        at = pl.ds(c * QK, QK)
        part = dot_nn(key_ref[2 * slot + head // 4, at, :], query_ref[HEADS * slot + head])
        part = part + bias_ref[head, at, :]
        into[at, :] = part
        return jnp.max(part.reshape(QK // 8, 8, positions), axis=0)

    def highest(tops):
        return jnp.max(functools.reduce(jnp.maximum, tops), axis=0, keepdims=True)

    def step(slot, head, slot_next, head_next, source, into, top):
        total = jnp.zeros((VROWS, positions), F32)
        tops = []
        for c in range(keys // PV):
            for k in range(PV // QK):
                tops.append(scores(slot_next, head_next, into, c * (PV // QK) + k))
            at = pl.ds(c * PV, PV)
            weight = jnp.exp2(source[at, :] - top).astype(BF16)
            total = total + dot_nn(value_ref[HEADS * slot + head, :, at], weight)
        att_ref[slot, pl.ds(pl.multiple_of(head * WIDTH, WIDTH), WIDTH), :] = (
            total[:WIDTH] / total[WIDTH : WIDTH + 1]
        )
        return highest(tops)

    pairs = HEADS // 2
    steps = sequences * pairs

    bias.second(0)
    bias.second(1)
    rows.second(0)
    bias.second(2)
    rows.second(1)
    bias.second(3)
    rows.second(2)
    bias_third(0)
    rows.second(3)
    bias_third(1)
    rows.second(4)
    bias_third(2)
    bias_third(3)
    rows.second(5)
    bias_fourth(0)
    bias_fourth(1)
    row_third(0)
    bias_fourth(2)
    bias_fourth(3)
    project(0)
    bias_done(0)
    bias_done(1)
    max_ref[...] = highest([scores(0, 0, even_ref, c) for c in range(keys // QK)])

    @pl.loop(0, steps)
    def _(it):
        following = jnp.minimum(it + 1, steps - 1)
        s, pair = it // pairs, lax.rem(it, pairs)
        s_next, pair_next = following // pairs, lax.rem(following, pairs)
        slot, slot_next = lax.rem(s, 2), lax.rem(s_next, 2)

        def at_step(k, *actions):
            @pl.when(it == k)
            def _():
                for action, n in actions:
                    action(n)

        at_step(0, (rows.second, 6))
        at_step(1, (row_third, 1), (bias_done, 2))
        at_step(2, (rows.second, 7), (bias_done, 3))
        at_step(4, (row_third, 2))
        at_step(6, (row_third, 3))
        at_step(9, (row_third, 4))
        at_step(12, (row_third, 5))
        at_step(15, (row_third, 6))
        at_step(18, (row_third, 7))

        @pl.when((pair == 0) & (it > 0))
        def _():
            send_columns(s - 1)

        @pl.when(pair_next == 0)
        def _():
            project(s_next)

        head = pair * 2
        top = step(slot, head, slot, head + 1, even_ref, odd_ref, max_ref[...])
        max_ref[...] = step(slot, head + 1, slot_next, pair_next * 2, odd_ref, even_ref, top)

        @pl.when(pair == pairs - 1)
        def _():
            own = rows_ref[s, own_spot, :]
            gates = jax.nn.sigmoid(dot_nn(own, switch_ref[1]) + shift_ref[...])
            attended = (att_ref[slot].T * gates).astype(BF16)
            mixed = x_ref[s].astype(F32) + dot_nn(attended, final_ref[...])
            mixed_ref[s] = mixed
            stage_ref[s] = mixed.astype(BF16)
            columns_ref[seq * sequences + s] = stage_ref[
                s, pl.ds(pl.multiple_of(seq * residues, residues), residues), :
            ]

    send_columns(sequences - 1)

    moved = columns_ref.at[pl.ds(0, sequences * (seq_count - 1))]
    every = pltpu.make_async_remote_copy(
        src_ref=moved,
        dst_ref=moved,
        send_sem=column_send,
        recv_sem=column_recv,
        device_id={"seq": twin},
        device_id_type=MESH,
    )
    every.wait_recv()
    column_phase(
        columns_ref, norm_v_ref, probe_v_ref, switch_v_ref, shift_v_ref, final_v_ref,
        back_ref,
        left_ref, right_ref, out_left_ref, out_right_ref, delta_ref, probe_t_ref, switch_t_ref,
        column_query_ref, column_att_ref,
        back_send, back_recv,
    )
    every.wait_send()

    @pl.loop(0, sequences)
    def _(n):
        rows.sent(n, *ROW_KINDS)

    @pl.loop(0, BIAS_PIECES)
    def _(n):
        bias.sent(n, *BIAS_KINDS)
        pair_copy(n, bias.core).wait_send()


def attention(
    x, prior, factor, norm, probe, switch, shift, final, norm_v, probe_v, switch_v, shift_v, final_v
):
    sequences, positions, depth = x.shape
    keys = positions * lax.axis_size("res")
    seq_count = lax.axis_size("seq")
    count, residues = sequences * seq_count, positions // seq_count
    part_size = residues // 2
    vmem = pl.BlockSpec(memory_space=VM)
    dma = pltpu.SemaphoreType.DMA
    return pl.pallas_call(
        row_kernel,
        out_shape=[
            jax.ShapeDtypeStruct(x.shape, F32),
            jax.ShapeDtypeStruct(x.shape, BF16),
        ],
        in_specs=[vmem, vmem, pl.BlockSpec(memory_space=pltpu.SMEM)] + [vmem] * 10,
        out_specs=[vmem, vmem],
        scratch_shapes=[
            VM((count, residues, depth), BF16),
            VM((sequences, positions, depth), BF16),
            VM((sequences, keys, depth), BF16),
            VM((HEADS, seq_count // 2, 2, HALF, positions), BF16),
            VM((HEADS, keys, positions), F32),
            VM((keys, positions), F32),
            VM((keys, positions), F32),
            VM((4, keys, HALF), BF16),
            VM((2 * HEADS, VROWS, keys), BF16),
            VM((2 * HEADS, HALF, positions), BF16),
            VM((depth, depth), BF16),
            VM((depth, depth), BF16),
            VM((2, depth, positions), F32),
            VM((1, positions), F32),
            VM((count * residues, HALF), F32),
            VM((count * residues, HALF), F32),
            VM((count * part_size, HALF), F32),
            VM((count * part_size, HALF), F32),
            VM((residues // part_size, count, part_size, depth), BF16),
            VM((8, HALF, 4 * count), BF16),
            VM((2, depth, 2 * count), F32),
            dma((sequences, 10)),
            dma((sequences, 10)),
            dma((BIAS_PIECES, 9)),
            dma((BIAS_PIECES, 9)),
            dma((BIAS_PIECES,)),
            dma((BIAS_PIECES,)),
            dma,
            dma,
            dma,
            dma,
        ],
        compiler_params=pltpu.CompilerParams(
            vmem_limit_bytes=66_000_000, collective_id=0, has_side_effects=True
        ),
    )(
        x, prior, factor, norm[None], probe, switch, shift[None], final,
        norm_v[None], probe_v, switch_v, shift_v[None], final_v,
    )


def column_phase(
    rows_ref, norm_ref, probe_ref, switch_ref, shift_ref, final_ref,
    back_ref,
    left_ref, right_ref, out_left_ref, out_right_ref, stage_ref, probe_t_ref, switch_t_ref,
    query_ref, att_ref,
    send_sem, recv_sem,
):
    count, residues, depth = rows_ref.shape
    seq = lax.axis_index("seq")
    seq_count = lax.axis_size("seq")
    sequences = back_ref.shape[0]
    part_size = stage_ref.shape[2]
    probe_t_ref[...] = probe_ref[0].astype(F32).T.astype(BF16)
    switch_t_ref[...] = switch_ref[0].astype(F32).T.astype(BF16)
    query_ref[...] = jnp.zeros_like(query_ref)
    scale = LOG2E / math.sqrt(WIDTH)
    step = 16

    @pl.loop(0, count // step)
    def _(i):
        part = rows_ref[pl.ds(pl.multiple_of(i * step, step), step)].astype(F32)
        rows = step * residues
        part = standardize(part.reshape(rows, depth), norm_ref[...])
        at = pl.ds(pl.multiple_of(i * rows, rows), rows)
        left_ref[at, :] = part[:, :HALF]
        right_ref[at, :] = part[:, HALF:]

    ones = jnp.ones((16, count), BF16)

    def attend(r, slot):
        normed = jnp.concatenate(
            [
                jnp.concatenate(
                    [
                        left_ref[pl.ds(r + k, count, stride=residues), :],
                        right_ref[pl.ds(r + k, count, stride=residues), :],
                    ],
                    axis=1,
                )
                for k in range(2)
            ],
            axis=0,
        ).astype(BF16)
        key = dot_nn(normed, probe_ref[1]).astype(BF16)
        query = (dot_nt(probe_t_ref[...], normed) * scale).astype(BF16)
        value = dot_nt(switch_t_ref[...], normed).astype(BF16)
        gates = jax.nn.sigmoid(dot_nn(normed, switch_ref[1]) + shift_ref[...])
        for k in range(2):
            mine = slice(k * count, (k + 1) * count)
            for half in range(2):
                spot = 4 * slot + 2 * k + half
                for h in range(4):
                    low = h * WIDTH
                    query_ref[spot, low : low + WIDTH, h * count : (h + 1) * count] = query[
                        half * HALF + low : half * HALF + low + WIDTH, mine
                    ]
                score = dot_nn(key[mine, half * HALF : (half + 1) * HALF], query_ref[spot])
                top = jnp.max(score, axis=0, keepdims=True)
                weight = jnp.exp2(score - top).astype(BF16)
                for h in range(0, 4, 2):
                    low = half * HALF + h * WIDTH
                    block = jnp.concatenate([value[low : low + 2 * WIDTH, mine], ones], axis=0)
                    total = dot_nn(block, weight[:, h * count : (h + 2) * count])
                    for j in range(2):
                        spread = slice(j * count, (j + 1) * count)
                        att_ref[
                            slot, low + j * WIDTH : low + (j + 1) * WIDTH, k * count : (k + 1) * count
                        ] = (
                            total[j * WIDTH : (j + 1) * WIDTH, spread]
                            / total[2 * WIDTH : 2 * WIDTH + 1, spread]
                        )
        attended = (att_ref[slot].T * gates).astype(BF16)
        return dot_nn(attended, final_ref[...])

    def back_copy(part, target):
        return pltpu.make_async_remote_copy(
            src_ref=stage_ref.at[part, pl.ds(target * sequences, sequences)],
            dst_ref=back_ref.at[
                :, pl.ds(pl.multiple_of(seq * residues + part * part_size, part_size), part_size), :
            ],
            send_sem=send_sem,
            recv_sem=recv_sem,
            device_id={"seq": target},
            device_id_type=MESH,
        )

    pairs = 2
    for part in range(residues // part_size):

        @pl.loop(0, part_size // (2 * pairs))
        def _(group):
            low = group * (2 * pairs)
            deltas = [attend(part * part_size + low + 2 * p, p) for p in range(pairs)]
            for p, delta in enumerate(deltas):
                for k in range(2):
                    spots = pl.ds(low + 2 * p + k, count, stride=part_size)
                    out_left_ref[spots, :] = delta[k * count : (k + 1) * count, :HALF]
                    out_right_ref[spots, :] = delta[k * count : (k + 1) * count, HALF:]

        @pl.loop(0, count // step)
        def _(i):
            rows = step * part_size
            at = pl.ds(pl.multiple_of(i * rows, rows), rows)
            block = jnp.concatenate([out_left_ref[at, :], out_right_ref[at, :]], axis=1)
            stage_ref[part, pl.ds(pl.multiple_of(i * step, step), step)] = block.astype(BF16).reshape(
                step, part_size, depth
            )

        @pl.loop(1, seq_count)
        def _(k):
            back_copy(part, lax.rem(seq + k, seq_count)).start()

        back_ref[
            :, pl.ds(pl.multiple_of(seq * residues + part * part_size, part_size), part_size), :
        ] = stage_ref[part, pl.ds(seq * sequences, sequences)]

    moved = back_ref.at[:, pl.ds(0, residues * (seq_count - 1)), :]
    every = pltpu.make_async_remote_copy(
        src_ref=moved,
        dst_ref=moved,
        send_sem=send_sem,
        recv_sem=recv_sem,
        device_id={"seq": lax.rem(seq + 1, seq_count)},
        device_id_type=MESH,
    )
    every.wait_send()
    every.wait_recv()


def shards(x, prior, factor, norm_h, probe_h, switch_h, shift_h, final_h, norm_v, probe_v, switch_v, shift_v, final_v):
    mixed, back = attention(
        x, prior, factor, norm_h, probe_h, switch_h, shift_h, final_h, norm_v, probe_v, switch_v, shift_v, final_v
    )
    return mixed + back.astype(F32)


def solution(mesh):
    placed = (P("seq", "res", None), P(None, "res", "seq")) + (P(),) * 11
    return jax.shard_map(
        shards, mesh=mesh, in_specs=placed, out_specs=P("seq", "res", None), check_vma=False
    )
```
